32 devices in a mesh: row: 2 (over core), col: 8 (over z, x), mp: 2 (over y).
Axes of the slice: x: 2, y: 2, z: 4, core: 2. Of those that a mesh axis runs over, the one named last changes fastest.
Arguments:
- video: bfloat16 [3, 4, 48, 3072], P(None, None, 'row', 'col'), may hold values from -6 to 6
- grad_tokens: bfloat16 [2, 4, 256, 1024], P(None, 'row', 'col', 'mp'), may hold values from -6 to 6
- weight: bfloat16 [3072, 1024], P(None, 'mp'), may hold values from -0.1875 to 0.1875
Outputs:
- video_grad: float32 [3, 4, 48, 3072], P(None, 'mp', 'row', 'col')
- weight_grad: float32 [3072, 1024], P(('row', 'col'), 'mp')
The draws below stay inside these ranges and needn't reach their ends.
All inputs are finite; a program needn't handle non-finite values.
Results may differ from the reference program's by a relative error of at most 0.0003.
Values may be sent and summed in bfloat16 or wider, within the bound.
No kernel may reach another device: no remote copies, remote signals or barrier semaphores. Data moves between devices by JAX's collectives and lax.ppermute only.
A program may use at most 64 MiB of HBM per device.

```python
import jax
import jax.numpy as jnp
from jax import lax

D = 1024
PATCH = 3072
TT = 2
FRAMES = 4
NTH = 4
NTW = 256
HEIGHT = 48
WIDTH = 3072


def shard_levels(rng, dims, split, smallest, largest):
    factor_of = 1.0
    for dim, shards_of in split:
        heights = jax.random.uniform(jax.random.fold_in(jax.random.fold_in(rng, 6), dim), (shards_of,), jnp.float32, smallest / len(split), largest / len(split))
        factor_of = factor_of * jnp.repeat(jnp.exp(heights), dims[dim] // shards_of).reshape((-1,) + (1,) * (len(dims) - 1 - dim))
    return factor_of


def gaussian(own_key, extent, spread, bound, cuts=(), kind=jnp.bfloat16):
    result = spread * jax.random.normal(own_key, extent, jnp.float32)
    if cuts:
        result = result * shard_levels(own_key, extent, cuts, -0.22, 0.18)
    return jnp.clip(result, -bound, bound).astype(kind)


def setup_inputs(seed: int = 0) -> dict:
    key_of = jax.random.split(jax.random.key(seed), 4)
    return {
        "video": gaussian(key_of[0], (3, FRAMES, HEIGHT, WIDTH), 1.0, 6.0, ((2, 2), (3, 8))),
        "grad_tokens": gaussian(key_of[1], (TT, NTH, NTW, D), 1.0, 6.0, ((1, 2), (2, 8), (3, 2))),
        "weight": gaussian(key_of[2], (PATCH, D), D ** -0.5, 0.1875, ((1, 2),)),
    }


def unfold_axis(ext, axis, count, stride, kernel):
    extra = max(0, 2 * stride - kernel)
    widths = [(0, 0)] * ext.ndim
    widths[axis] = (0, extra)
    ext = jnp.pad(ext, widths)
    lower = lax.slice_in_dim(ext, 0, count * stride, axis=axis)
    upper = lax.slice_in_dim(ext, stride, stride + count * stride, axis=axis)
    shaped = ext.shape[:axis] + (count, stride) + ext.shape[axis + 1:]
    lower = lower.reshape(shaped)
    upper = lax.slice_in_dim(upper.reshape(shaped), 0, kernel - stride, axis=axis + 1)
    return jnp.concatenate([lower, upper], axis=axis + 1)

def fold_axis(pieces, axis, stride, kernel):
    count = pieces.shape[axis]
    lower = lax.slice_in_dim(pieces, 0, stride, axis=axis + 1)
    upper = lax.slice_in_dim(pieces, stride, kernel, axis=axis + 1)
    pad_lower = [(0, 0)] * pieces.ndim
    pad_upper = [(0, 0)] * pieces.ndim
    pad_lower[axis] = (0, 1)
    pad_upper[axis] = (1, 0)
    pad_upper[axis + 1] = (0, 2 * stride - kernel)
    total = jnp.pad(lower, pad_lower) + jnp.pad(upper, pad_upper)
    merged = total.reshape(pieces.shape[:axis] + ((count + 1) * stride,) + pieces.shape[axis + 2:])
    return lax.slice_in_dim(merged, 0, count * stride + kernel - stride, axis=axis)

def reference(video, grad_tokens, weight):
    padded = jnp.pad(video, ((0, 0), (1, 1), (2, 2), (2, 2)))
    steps, rows, cols, width = grad_tokens.shape
    patch = weight.shape[0]
    zero = jnp.int32(0)
    field = jnp.zeros((3, 2 * steps + 2, padded.shape[2], padded.shape[3]), jnp.float32)
    weight_sum = jnp.zeros((patch, width), jnp.float32)

    def one_step(carry, index):
        weight_sum, field = carry
        start = (2 * index).astype(jnp.int32)
        frames = lax.dynamic_slice_in_dim(padded, start, 4, 1)
        pieces = unfold_axis(unfold_axis(frames, 2, rows, 12, 16), 4, cols, 12, 16)
        pieces = pieces.transpose(2, 4, 0, 1, 3, 5).reshape(rows * cols, patch)
        tokens = lax.dynamic_index_in_dim(grad_tokens, index, 0, keepdims=False).reshape(rows * cols, width)
        weight_sum = weight_sum + lax.dot_general(pieces, tokens, (((0,), (0,)), ((), ())), preferred_element_type=jnp.float32)
        grads = lax.dot_general(tokens, weight, (((1,), (1,)), ((), ())), preferred_element_type=jnp.float32)
        grads = grads.reshape(rows, cols, 3, 4, 16, 16).transpose(2, 3, 0, 4, 1, 5)
        grads = fold_axis(fold_axis(grads, 4, 12, 16), 2, 12, 16)
        old = lax.dynamic_slice(field, (zero, start, zero, zero), grads.shape)
        field = lax.dynamic_update_slice(field, old + grads, (zero, start, zero, zero))
        return ((weight_sum, field), None)
    (weight_sum, field), unused = lax.scan(one_step, (weight_sum, field), jnp.arange(steps, dtype=jnp.int32))
    video_grad = field[:, 1:-1, 2:-2, 2:-2]
    weight_grad = weight_sum * lax.rsqrt(jnp.float32(steps * rows * cols))
    return (video_grad, weight_grad)
```

```python
import functools

import jax
import jax.numpy as jnp
import numpy as np
from jax import lax
from jax.experimental import pallas as pl
from jax.experimental.pallas import tpu as pltpu
from jax.sharding import PartitionSpec as P

KT, KS, ST, SS = 4, 16, 2, 12
LAP = (KS - SS) // 2

VMEM = pltpu.VMEM


def swap(x, axis, bit):
    n = lax.axis_size(axis)
    return lax.ppermute(x, axis, [(i, i ^ bit) for i in range(n)])


def shift(x, axis, by):
    n = lax.axis_size(axis)
    return lax.ppermute(x, axis, [(i, i + by) for i in range(n) if 0 <= i + by < n])


def rotate(x, axis, by):
    n = lax.axis_size(axis)
    return lax.ppermute(x, axis, [(i, (i + by) % n) for i in range(n)])


def fold_matrix(cols):
    width = SS * cols
    m = np.zeros((KS * cols + 128, width), np.float32)
    for e in range(KS):
        for j in range(cols):
            x = SS * j + e - LAP
            if 0 <= x < width:
                m[e * cols + j, x] = 1
    for k in range(LAP):
        m[KS * cols + 16 * k, k] = 1
        m[KS * cols + 16 * (LAP + k) + 4, width - LAP + k] = 1
    return jnp.asarray(m, jnp.bfloat16)


def unfold_matrix(cols):
    width = SS * cols
    m = np.zeros((width + 256, KS * cols), np.float32)
    for e in range(KS):
        for j in range(cols):
            m[128 + SS * j + e - LAP, e * cols + j] = 1
    return jnp.asarray(m, jnp.bfloat16)


def video_kernel(dims, w_ref, g_ref, edge_ref, s_ref, *refs):
    steps, rows, cols, parts, split = dims
    keep_ref, send_ref = refs[:2]
    halos = refs[2 : len(refs) - 2]
    p_ref, f_ref = refs[len(refs) - 2 :]
    tokens = jnp.concatenate([g_ref[...], edge_ref[...]], axis=0)
    p = lax.dot_general(
        w_ref[...], tokens, (((1,), (1,)), ((), ())), preferred_element_type=jnp.float32
    )
    count = steps * rows * cols
    entries = KT * KS
    tiles = count // 128
    for k in range(tiles):
        p_ref[k] = p[:, k * 128 : (k + 1) * 128]
    p_ref[tiles, :, :16] = p[:, count:]
    strided = lambda k, e: p_ref.at[k][pl.ds(e, entries, stride=KS), :]
    by_e = [[strided(k, e) for k in range(tiles)] for e in range(KS)]
    by_e = [jnp.concatenate(v, axis=1) if tiles > 1 else v[0] for v in by_e]
    edges = [strided(tiles, e)[:, :16] for e in (KS - LAP, KS - LAP + 1, 0, 1)]
    edges = jnp.concatenate(edges + [jnp.zeros((entries, 64), jnp.float32)], axis=1)
    lane = lax.broadcasted_iota(jnp.int32, (entries, 128), 1)
    canon = (lane == 0) | (lane == 16) | (lane == 36) | (lane == 52)
    f_ref[...] = jnp.zeros_like(f_ref)
    for t in range(steps):
        for i in range(rows):
            ti = t * rows + i
            edge = edges if ti == 0 else pltpu.roll(edges, 128 - ti, 1)
            q = jnp.concatenate(
                [v[:, ti * cols : (ti + 1) * cols] for v in by_e] + [jnp.where(canon, edge, 0.0)],
                axis=1,
            )
            for a in range(KT):
                f = ST * t + a - 1
                if 0 <= f < ST * steps:
                    top = 8 - LAP + SS * i
                    f_ref[f, top : top + KS, :] += q[a * KS : (a + 1) * KS]
    frames = ST * steps
    tall = f_ref.shape[1]
    full = f_ref[...].reshape(frames * tall, f_ref.shape[2])
    high = full.astype(jnp.bfloat16)
    low = (full - high.astype(jnp.float32)).astype(jnp.bfloat16)
    dot = functools.partial(jnp.dot, preferred_element_type=jnp.float32)
    out = (dot(high, s_ref[...]) + dot(low, s_ref[...])).reshape(frames, tall, -1)
    height = SS * rows
    inner = out[:, 8 : 8 + height]
    above = out[:, 8 - LAP : 8]
    below = out[:, 8 + height : 8 + height + LAP]
    me = lax.axis_index("mp")
    per = frames // parts
    for g in range(parts):
        block = inner[g * per : (g + 1) * per]

        @pl.when(me == g)
        def _():
            keep_ref[0] = block

        for s in range(1, parts):

            @pl.when(lax.rem(me + s, parts) == g)
            def _():
                send_ref[s - 1, 0] = block

    if split == 2:
        halos[0][0] = jnp.where(lax.axis_index("row") == 0, below, above)
    else:
        halos[0][0] = above
        halos[1][0] = below


def video_partials(weight, flat, edge, dims, channels):
    steps, rows, cols, parts, split = dims
    half = weight.shape[1]
    patch = weight.shape[0] // channels
    frames = ST * steps
    per = frames // parts
    height, width = SS * rows, SS * cols
    table = fold_matrix(cols)
    tall = -(-(8 + height + LAP) // 8) * 8
    halo = jax.ShapeDtypeStruct((channels, frames, LAP, width), jnp.float32)
    whole = lambda x: pl.BlockSpec(x.shape, lambda c: (0,) * x.ndim)
    halo_spec = pl.BlockSpec((1, frames, LAP, width), lambda c: (c, 0, 0, 0))
    sides = 1 if split == 2 else 2
    return pl.pallas_call(
        functools.partial(video_kernel, dims),
        grid=(channels,),
        in_specs=[
            pl.BlockSpec((patch, half), lambda c: (c, 0)),
            whole(flat),
            whole(edge),
            whole(table),
        ],
        out_specs=[
            pl.BlockSpec((1, per, height, width), lambda c: (c, 0, 0, 0)),
            pl.BlockSpec((parts - 1, 1, per, height, width), lambda c: (0, c, 0, 0, 0)),
        ]
        + [halo_spec] * sides,
        out_shape=[
            jax.ShapeDtypeStruct((channels, per, height, width), jnp.float32),
            jax.ShapeDtypeStruct((parts - 1, channels, per, height, width), jnp.float32),
        ]
        + [halo] * sides,
        scratch_shapes=[
            VMEM((flat.shape[0] // 128 + 1, patch, 128), jnp.float32),
            VMEM((frames, tall, KS * cols + 128), jnp.float32),
        ],
        cost_estimate=pl.CostEstimate(
            flops=2 * weight.size * flat.shape[0] * 2, bytes_accessed=2 * weight.size, transcendentals=0
        ),
        name="video_partials",
    )(weight, flat, edge, table)


def slab_kernel(sel_ref, selh_ref, video_ref, halo_ref, *outs):
    dot = functools.partial(jnp.dot, preferred_element_type=jnp.float32)
    rows = dot(sel_ref[...], video_ref[...]) + dot(selh_ref[...], halo_ref[...])
    rows = rows.astype(jnp.bfloat16)
    size = outs[0].shape[0]
    for k, out in enumerate(outs):
        out[...] = rows[k * size : (k + 1) * size]


def weight_kernel(dims, *refs):
    groups, cols, units = dims
    nc = lax.axis_size("col")
    slabs, refs = refs[:nc], refs[nc:]
    near_ref, far_ref, s_ref, out_ref, x_ref, g_ref, a_ref, m_ref = refs
    me = lax.axis_index("col")
    width = SS * cols
    tall = groups * units
    x_ref[:, :128] = jnp.zeros((tall, 128), x_ref.dtype)
    x_ref[:, 128 + nc * width :] = jnp.zeros((tall, 128), x_ref.dtype)
    for s in range(nc):
        at = pl.multiple_of(128 + jnp.bitwise_xor(me, s) * width, 128)
        x_ref[:, pl.ds(at, width)] = slabs[s][...]
    for k, ref in enumerate((near_ref, far_ref)):
        for n in range(nc // 2):
            src = jnp.bitwise_xor(me, doubled(nc, n) + k)
            for ti in range(groups):
                at = pl.multiple_of(ti * nc * cols + src * cols, cols)
                g_ref[pl.ds(at, cols), :] = ref[n, ti * cols : (ti + 1) * cols, :]
    wide = jnp.concatenate([x_ref[:, c * width : (c + 1) * width + 256] for c in range(nc)], axis=0)
    u = jnp.dot(wide, s_ref[...], preferred_element_type=jnp.float32)
    pack = 128 // cols
    for cg in range(nc // pack):
        for e in range(0, KS, 2):
            pair = [
                jnp.concatenate(
                    [
                        u[(cg * pack + c) * tall : (cg * pack + c + 1) * tall, (e + d) * cols : (e + d + 1) * cols]
                        for c in range(pack)
                    ],
                    axis=1,
                )
                for d in range(2)
            ]
            for ti in range(groups):
                both = jnp.concatenate([v[ti * units : (ti + 1) * units] for v in pair], axis=0)
                at = ti * nc * cols + cg * 128
                a_ref[e * units : (e + 2) * units, at : at + 128] = both.astype(a_ref.dtype)
    m = jnp.dot(a_ref[...], g_ref[...], preferred_element_type=jnp.float32)
    for k in range(m_ref.shape[0]):
        for e in range(KS):
            m_ref.at[k][pl.ds(e, units, stride=KS), :] = m[e * units : (e + 1) * units, k * 128 : (k + 1) * 128]
        out_ref[:, k * 128 : (k + 1) * 128] = m_ref[k]


def doubled(nc, n):
    off, bit, k = 0, nc // 2, 0
    while bit > 1:
        if (n >> k) & 1:
            off ^= bit
        bit //= 2
        k += 1
    return off


def shards(video, grad_tokens, weight):
    steps, rows, cols, half = grad_tokens.shape
    channels, frames, height, width = video.shape
    patch = weight.shape[0]
    nr, nc, nm = lax.axis_size("row"), lax.axis_size("col"), lax.axis_size("mp")
    r, c = lax.axis_index("row"), lax.axis_index("col")
    groups = steps * rows
    count = groups * cols
    flat = grad_tokens.reshape(count, half)
    dims = (steps, rows, cols, nm, nr)

    top, bottom = video[:, :, :LAP], video[:, :, height - LAP :]
    if nr == 2:
        halo = swap(jnp.where(r == 0, bottom, top), "row", 1).reshape(-1, width)
    else:
        halo = jnp.concatenate([shift(bottom, "row", 1), shift(top, "row", -1)], axis=0).reshape(-1, width)

    left = shift(grad_tokens[:, :, -1], "col", 1).reshape(groups, half)
    right = shift(grad_tokens[:, :, 0], "col", -1).reshape(groups, half)
    edge = jnp.concatenate([left, right, jnp.zeros((16 - 2 * groups, half), left.dtype)], axis=0)

    near = flat[None]
    bit = nc // 2
    while bit > 1:
        near = jnp.concatenate([near, swap(near, "col", bit)], axis=0)
        bit //= 2
    far = swap(near, "col", 1)

    block = patch // (nr * nc)
    touched = max((k * block % KS + block + KS - 1) // KS for k in range(nr * nc))
    units = nr * touched
    n = lax.broadcasted_iota(jnp.int32, (nc * groups * units, 1), 0)
    q = n % touched
    rho = n // touched % nr
    i = n // units % rows
    t = n // (units * rows) % steps
    s = n // (units * groups)
    owner = (r + rho) % nr * nc + jnp.bitwise_xor(c, s)
    triple = owner * block // KS + q
    ch, a, b = triple // (KT * KS), triple // KS % KT, triple % KS
    f = ST * t + a - 1
    y = SS * i + b - LAP
    ok = (f >= 0) & (f < frames) & (triple < patch // KS)
    image = ch * frames + f
    inside = (y >= 0) & (y < height)
    pick = jnp.where(ok & inside, image * height + y, -1)
    if nr == 2:
        side = ((y < 0) & (r == 1)) | ((y >= height) & (r == 0))
        base = image * LAP
    else:
        side = ~inside
        base = image * LAP + jnp.where(y < 0, 0, channels * frames * LAP)
    pick_halo = jnp.where(ok & side, base + jnp.where(y < 0, y + LAP, y - height), -1)
    one_hot = lambda idx, size: (idx == lax.broadcasted_iota(jnp.int32, (1, size), 1)).astype(video.dtype)
    sel = one_hot(pick, channels * frames * height)
    sel_halo = one_hot(pick_halo, halo.shape[0])
    slabs = pl.pallas_call(
        slab_kernel,
        out_shape=[jax.ShapeDtypeStruct((groups * units, width), video.dtype)] * nc,
        cost_estimate=pl.CostEstimate(flops=2 * sel.size * width, bytes_accessed=4 * sel.size, transcendentals=0),
        name="slabs",
    )(sel, sel_halo, video.reshape(-1, width), halo)
    slabs = [slabs[0]] + [swap(slabs[k], "col", k) for k in range(1, nc)]

    keep, send, *rims = video_partials(weight, flat, edge, dims, channels)
    if nr == 2:
        rim = swap(rims[0], "row", 1)
        zero = jnp.zeros_like(rim)
        from_above = jnp.where(r == 1, rim, zero)
        from_below = jnp.where(r == 0, rim, zero)
    else:
        from_below = shift(rims[0], "row", -1)
        from_above = shift(rims[1], "row", 1)
    middle = jnp.zeros((channels, frames, height - 2 * LAP, width), jnp.float32)
    extra = jnp.concatenate([from_above, middle, from_below], axis=2)
    extra = extra.reshape(channels, nm, frames // nm, height, width)
    m = lax.axis_index("mp")
    part = lambda s: lax.dynamic_index_in_dim(extra, (m + s) % nm, 1, keepdims=False)
    video_grad = keep + part(0)
    for s in range(1, nm):
        video_grad = video_grad + rotate(send[s - 1] + part(s), "mp", s)

    table = unfold_matrix(cols)
    out = pl.pallas_call(
        functools.partial(weight_kernel, (groups, cols, units)),
        out_shape=jax.ShapeDtypeStruct((units * KS, half), jnp.float32),
        scratch_shapes=[
            VMEM((groups * units, nc * width + 256), video.dtype),
            VMEM((groups * nc * cols, half), video.dtype),
            VMEM((KS * units, groups * nc * cols), video.dtype),
            VMEM((half // 128, KS * units, 128), jnp.float32),
        ],
        cost_estimate=pl.CostEstimate(
            flops=4 * units * KS * groups * nc * cols * half, bytes_accessed=1 << 21, transcendentals=0
        ),
        name="weight_partials",
    )(*slabs, near, far, table)
    total = None
    for s in range(nr):
        own = (r + s) % nr * nc + c
        start = s * touched * KS + own * block % KS
        if block % KS:
            mine = lax.dynamic_slice_in_dim(out, start, block, 0)
        else:
            mine = lax.slice_in_dim(out, s * touched * KS, s * touched * KS + block, axis=0)
        total = mine if s == 0 else total + rotate(mine, "row", s)
    weight_grad = total * lax.rsqrt(jnp.float32(count * nr * nc))
    return video_grad, weight_grad


def solution(mesh):
    return jax.shard_map(
        shards,
        mesh=mesh,
        in_specs=(P(None, None, "row", "col"), P(None, "row", "col", "mp"), P(None, "mp")),
        out_specs=(P(None, "mp", "row", "col"), P(("row", "col"), "mp")),
        check_vma=False,
    )
```

```python
import functools

import jax
import jax.numpy as jnp
import numpy as np
from jax import lax
from jax.experimental import pallas as pl
from jax.experimental.pallas import tpu as pltpu
from jax.sharding import PartitionSpec as P

KT, KS, ST, SS = 4, 16, 2, 12
LAP = (KS - SS) // 2

VMEM = pltpu.VMEM


def grant(mib):
    return pltpu.CompilerParams(vmem_limit_bytes=mib << 20)


def swap(x, axis, bit):
    n = lax.axis_size(axis)
    return lax.ppermute(x, axis, [(i, i ^ bit) for i in range(n)])


def shift(x, axis, by):
    n = lax.axis_size(axis)
    return lax.ppermute(x, axis, [(i, i + by) for i in range(n) if 0 <= i + by < n])


def rotate(x, axis, by):
    n = lax.axis_size(axis)
    return lax.ppermute(x, axis, [(i, (i + by) % n) for i in range(n)])


def grid_of(rows, columns):
    return (
        lax.broadcasted_iota(jnp.int32, (rows, columns), 0),
        lax.broadcasted_iota(jnp.int32, (rows, columns), 1),
    )


def zero_one(mask):
    return jnp.where(mask, 1.0, 0.0).astype(jnp.bfloat16)


def fold_matrix(cols):
    width = SS * cols
    n, x = grid_of(KS * cols, width)
    inner = zero_one(SS * lax.rem(n, cols) + lax.div(n, cols) - LAP == x)
    n, x = grid_of(128, width)
    edge = (x < LAP) & (n == 16 * x) | (x >= width - LAP) & (n == 16 * (x - width + 2 * LAP) + 4)
    return jnp.concatenate([inner, zero_one(edge)], axis=0)


def unfold_matrix(cols):
    width = SS * cols
    x, n = grid_of(width + 128, KS * cols)
    x = jnp.where(x < width + 64, x, x - width - 128)
    return zero_one(SS * lax.rem(n, cols) + lax.div(n, cols) - LAP == x)


def edge_rows(groups, cols, first):
    k, n = grid_of(16, groups * cols)
    firsts = (k >= groups) & (k < 2 * groups) & (n == (k - groups) * cols)
    lasts = (k < groups) & (n == k * cols + cols - 1)
    return zero_one(firsts & first | lasts & jnp.logical_not(first))


def lap_rows(images, height, lap, at):
    k, n = grid_of(lap, images * height)
    return zero_one((k < images * LAP) & (n == lax.div(k, LAP) * height + lax.rem(k, LAP) + at))


def row_table(channels, frames, height, steps, rows, nr, nc, block, touched):
    inside, lap = channels * frames * height, halo_rows(channels, frames)
    m = np.zeros((nc, steps, rows, nr, touched, inside + 2 * lap), np.float32)
    for c, t, i, r, q in np.ndindex(*m.shape[:-1]):
        triple = (r * nc + c) * block // KS + q
        ch, a, b = triple // (KT * KS), triple // KS % KT, triple % KS
        f, y = ST * t + a - 1, SS * i + b - LAP
        if ch < channels and 0 <= f < frames:
            image = ch * frames + f
            if y < 0:
                k = inside + image * LAP + y + LAP
            elif y >= height:
                k = inside + lap + image * LAP + y - height
            else:
                k = image * height + y
            m[c, t, i, r, q, k] = 1
    return jnp.asarray(m.reshape(-1, m.shape[-1]), jnp.bfloat16)


def halo_rows(channels, frames):
    return -(-channels * frames * LAP // 16) * 16


def exact(a, b):
    return jnp.dot(a, b, preferred_element_type=jnp.float32).astype(jnp.bfloat16)


def even_column():
    return lax.rem(lax.axis_index("col"), 2) == 0


def prep_kernel(dims, video_ref, flat_ref, table_ref, video_out, flat_out, table_out, edge_ref, *refs):
    split, images, height, groups, cols = dims
    halos, sem = refs[:-1], refs[-1]
    pairs = ((flat_ref, flat_out), (video_ref, video_out), (table_ref, table_out))
    moves = [pltpu.make_async_copy(a, b, sem.at[k]) for k, (a, b) in enumerate(pairs)]
    for move in moves:
        move.start()
    picked = edge_rows(groups, cols, even_column())
    lap = halos[0].shape[0]
    if split == 2:
        at = jnp.where(lax.axis_index("row") == 0, height - LAP, 0)
        rows = [lap_rows(images, height, lap, at)]
    else:
        rows = [lap_rows(images, height, lap, at) for at in (0, height - LAP)]
    moves[0].wait()
    edge_ref[...] = exact(picked, flat_out[...])
    moves[1].wait()
    for row, halo in zip(rows, halos):
        halo[...] = exact(row, video_out[...])
    moves[2].wait()


def slab_kernel(split, table_ref, video_ref, weight_ref, *refs):
    halos, out_ref, weight_out, v_ref, rows_ref, sem = refs[:-5], *refs[-5:]
    move = pltpu.make_async_copy(weight_ref, weight_out, sem.at[0])
    move.start()
    inside, lap = video_ref.shape[0], halos[0].shape[0]
    v_ref[:inside] = video_ref[...]
    if split == 2:
        row = lax.axis_index("row")
        halo = halos[0][...]
        zero = jnp.zeros_like(halo)
        v_ref[inside : inside + lap] = zero
        v_ref[inside + lap :] = zero

        @pl.when(row == 1)
        def _():
            v_ref[inside : inside + lap] = halo

        @pl.when(row == 0)
        def _():
            v_ref[inside + lap :] = halo
    else:
        v_ref[inside : inside + lap] = halos[0][...]
        v_ref[inside + lap :] = halos[1][...]
    size = out_ref.shape[1]
    moves = [move]
    for k in range(out_ref.shape[0]):
        rows_ref[k] = exact(table_ref[k * size : (k + 1) * size], v_ref[...])
        moves.append(pltpu.make_async_copy(rows_ref.at[k], out_ref.at[k], sem.at[k + 1]))
        moves[-1].start()
    for move in moves:
        move.wait()


def video_kernel(dims, w_ref, g_ref, beside_ref, edge_ref, *refs):
    steps, rows, cols, parts, split = dims
    keep_ref, send_ref = refs[:2]
    halos = refs[2:-4]
    p_ref, f_ref, s_ref, t_ref = refs[-4:]
    ch = pl.program_id(0)
    count = steps * rows * cols

    @pl.when(ch == 0)
    def _():
        s_ref[...] = fold_matrix(cols)
        t_ref[:count] = g_ref[...]
        picked = edge_rows(steps * rows, cols, even_column())
        t_ref[count:] = exact(picked, beside_ref[...]) + edge_ref[...]

    patch = p_ref.shape[1]
    p = lax.dot_general(
        w_ref[pl.ds(pl.multiple_of(ch * patch, patch), patch), :],
        t_ref[...],
        (((1,), (1,)), ((), ())),
        preferred_element_type=jnp.float32,
    )
    entries = KT * KS
    tiles = count // 128
    for k in range(tiles):
        p_ref[k] = p[:, k * 128 : (k + 1) * 128]
    p_ref[tiles, :, :16] = p[:, count:]
    strided = lambda k, e: p_ref.at[k][pl.ds(e, entries, stride=KS), :]
    by_e = [[strided(k, e) for k in range(tiles)] for e in range(KS)]
    by_e = [jnp.concatenate(v, axis=1) if tiles > 1 else v[0] for v in by_e]
    edges = [strided(tiles, e)[:, :16] for e in (KS - LAP, KS - LAP + 1, 0, 1)]
    edges = jnp.concatenate(edges + [jnp.zeros((entries, 64), jnp.float32)], axis=1)
    lane = lax.broadcasted_iota(jnp.int32, (entries, 128), 1)
    canon = (lane == 0) | (lane == 16) | (lane == 36) | (lane == 52)
    f_ref[...] = jnp.zeros_like(f_ref)
    for t in range(steps):
        for i in range(rows):
            ti = t * rows + i
            edge = edges if ti == 0 else pltpu.roll(edges, 128 - ti, 1)
            q = jnp.concatenate(
                [v[:, ti * cols : (ti + 1) * cols] for v in by_e] + [jnp.where(canon, edge, 0.0)],
                axis=1,
            )
            for a in range(KT):
                f = ST * t + a - 1
                if 0 <= f < ST * steps:
                    top = 8 - LAP + SS * i
                    f_ref[f, top : top + KS, :] += q[a * KS : (a + 1) * KS]
    frames = ST * steps
    tall = f_ref.shape[1]
    full = f_ref[...].reshape(frames * tall, f_ref.shape[2])
    high = full.astype(jnp.bfloat16)
    low = (full - high.astype(jnp.float32)).astype(jnp.bfloat16)
    dot = functools.partial(jnp.dot, preferred_element_type=jnp.float32)
    out = (dot(high, s_ref[...]) + dot(low, s_ref[...])).reshape(frames, tall, -1)
    height = SS * rows
    inner = out[:, 8 : 8 + height]
    above = out[:, 8 - LAP : 8]
    below = out[:, 8 + height : 8 + height + LAP]
    me = lax.axis_index("mp")
    per = frames // parts
    for g in range(parts):
        block = inner[g * per : (g + 1) * per]

        @pl.when(me == g)
        def _():
            keep_ref[ch] = block

        for s in range(1, parts):

            @pl.when(lax.rem(me + s, parts) == g)
            def _():
                send_ref[s - 1, ch] = block

    if split == 2:
        halos[0][ch] = jnp.where(lax.axis_index("row") == 0, below, above)
    else:
        halos[0][ch] = above
        halos[1][ch] = below


def video_partials(weight, flat, beside, edge, dims, channels):
    steps, rows, cols, parts, split = dims
    half = weight.shape[1]
    patch = weight.shape[0] // channels
    frames = ST * steps
    per = frames // parts
    height, width = SS * rows, SS * cols
    tall = -(-(8 + height + LAP) // 8) * 8
    sides = 1 if split == 2 else 2
    f32 = lambda *shape: jax.ShapeDtypeStruct(shape, jnp.float32)
    spec = pl.BlockSpec(memory_space=VMEM)
    return pl.pallas_call(
        functools.partial(video_kernel, dims),
        grid=(channels,),
        in_specs=[spec] * 4,
        out_specs=[spec] * (2 + sides),
        out_shape=[f32(channels, per, height, width), f32(parts - 1, channels, per, height, width)]
        + [f32(channels, frames, LAP, width)] * sides,
        scratch_shapes=[
            VMEM((flat.shape[0] // 128 + 1, patch, 128), jnp.float32),
            VMEM((frames, tall, KS * cols + 128), jnp.float32),
            VMEM((KS * cols + 128, width), flat.dtype),
            VMEM((flat.shape[0] + 16, half), flat.dtype),
        ],
        cost_estimate=pl.CostEstimate(
            flops=4 * weight.size * flat.shape[0], bytes_accessed=2 * weight.size, transcendentals=0
        ),
        compiler_params=grant(14),
        name="video_partials",
    )(weight, flat, beside, edge)


def rim_kernel(dims, keep_ref, send_ref, *refs):
    parts, split = dims
    rims, (keep_out, send_out) = refs[:-2], refs[-2:]
    per, height = keep_ref.shape[1:3]
    me, row = lax.axis_index("mp"), lax.axis_index("row")
    for s in range(parts):
        src = keep_ref if s == 0 else send_ref.at[s - 1]
        out = keep_out if s == 0 else send_out.at[s - 1]
        out[...] = src[...]
        at = pl.ds(lax.rem(me + s, parts) * per, per)
        if split == 2:

            @pl.when(row == 1)
            def _():
                out[:, :, :LAP] += rims[0][:, at]

            @pl.when(row == 0)
            def _():
                out[:, :, height - LAP :] += rims[0][:, at]
        else:
            out[:, :, :LAP] += rims[0][:, at]
            out[:, :, height - LAP :] += rims[1][:, at]


def weight_kernel(dims, offsets, slab_ref, *refs):
    groups, cols, units, share, pieces = dims
    pieces, refs = refs[:pieces], refs[pieces:]
    nr, nc = lax.axis_size("row"), lax.axis_size("col")
    outs, (a_ref, m_ref) = refs[:-2], refs[-2:]
    me = lax.axis_index("col")
    width = SS * cols
    tall = groups * units
    half = m_ref.shape[0] * 128
    lane = lax.broadcasted_iota(jnp.int32, (tall, 128), 1)
    order = [jnp.bitwise_xor(me, o + h) for h in range(2) for o in offsets]
    wide = []
    for c in order:
        mine = slab_ref[c]
        before = slab_ref[jnp.maximum(c - 1, 0)][:, width - 128 :].astype(jnp.float32)
        after = slab_ref[jnp.minimum(c + 1, nc - 1)][:, :128].astype(jnp.float32)
        mixed = jnp.where((lane >= 128 - LAP) & (c > 0), before, 0.0)
        mixed = jnp.where((lane < LAP) & (c < nc - 1), after, mixed)
        wide.append(jnp.concatenate([mine, mixed.astype(mine.dtype)], axis=1))
    u = jnp.dot(jnp.concatenate(wide, axis=0), unfold_matrix(cols), preferred_element_type=jnp.float32)
    pack = 128 // cols
    for cg in range(nc // pack):
        for e in range(0, KS, 2):
            pair = [
                jnp.concatenate(
                    [
                        u[(cg * pack + c) * tall : (cg * pack + c + 1) * tall, (e + d) * cols : (e + d + 1) * cols]
                        for c in range(pack)
                    ],
                    axis=1,
                )
                for d in range(2)
            ]
            for ti in range(groups):
                both = jnp.concatenate([v[ti * units : (ti + 1) * units] for v in pair], axis=0)
                at = ti * nc * cols + cg * 128
                a_ref[e * units : (e + 2) * units, at : at + 128] = both.astype(a_ref.dtype)
    tokens = []
    for ti in range(groups):
        for ref in pieces:
            tokens.append(ref[:, ti * cols : (ti + 1) * cols, :].reshape(-1, half))
    m = jnp.dot(a_ref[...], jnp.concatenate(tokens, axis=0), preferred_element_type=jnp.float32)
    for k in range(m_ref.shape[0]):
        for e in range(KS):
            m_ref.at[k][pl.ds(e, units, stride=KS), :] = m[e * units : (e + 1) * units, k * 128 : (k + 1) * 128]
    row = lax.axis_index("row")
    for s, out in enumerate(outs):
        at = pl.multiple_of(lax.rem(row + s, nr) * share, 8)
        for k in range(m_ref.shape[0]):
            out[:, k * 128 : (k + 1) * 128] = m_ref[k, pl.ds(at, share), :]


def joined(parts):
    return parts[0] if len(parts) == 1 else jnp.concatenate(parts, axis=0)


def outside(x):
    return pltpu.with_memory_space_constraint(x, pltpu.HBM)


def call(kernel, args, outs, mib, scratch=(), hbm=(), out_hbm=(), flops=1 << 20):
    space = lambda k, hbm: pltpu.HBM if k in hbm else VMEM
    return pl.pallas_call(
        kernel,
        in_specs=[pl.BlockSpec(memory_space=space(k, hbm)) for k in range(len(args))],
        out_specs=[pl.BlockSpec(memory_space=space(k, out_hbm)) for k in range(len(outs))],
        out_shape=outs,
        scratch_shapes=scratch,
        cost_estimate=pl.CostEstimate(flops=flops, bytes_accessed=1 << 20, transcendentals=0),
        compiler_params=grant(mib),
    )(*args)


def both_gradients(video, grad_tokens, weight):
    steps, rows, cols, half = grad_tokens.shape
    channels, frames, height, width = video.shape
    patch = weight.shape[0]
    nr, nc, nm = lax.axis_size("row"), lax.axis_size("col"), lax.axis_size("mp")
    r, c = lax.axis_index("row"), lax.axis_index("col")
    groups = steps * rows
    count = groups * cols
    flat = grad_tokens.reshape(count, half)
    pixels = video.reshape(-1, width)
    dims = (steps, rows, cols, nm, nr)
    images = channels * frames
    lap = halo_rows(channels, frames)
    block = patch // (nr * nc)
    touched = max((k * block % KS + block + KS - 1) // KS for k in range(nr * nc))
    units = nr * touched
    bf16 = lambda *shape: jax.ShapeDtypeStruct(shape, video.dtype)
    f32 = lambda *shape: jax.ShapeDtypeStruct(shape, jnp.float32)

    table = row_table(channels, frames, height, steps, rows, nr, nc, block, touched)
    pixels, tokens, table, edge, *halos = call(
        functools.partial(prep_kernel, (nr, images, height, groups, cols)),
        (outside(pixels), outside(flat), outside(table)),
        [bf16(*pixels.shape), bf16(*flat.shape), bf16(*table.shape), bf16(16, half)]
        + [bf16(lap, width)] * (1 if nr == 2 else 2),
        6,
        scratch=[pltpu.SemaphoreType.DMA((3,))],
        hbm=(0, 1, 2),
    )
    if nr == 2:
        halos = [swap(halos[0], "row", 1)]
    else:
        halos = [shift(halos[1], "row", 1), shift(halos[0], "row", -1)]

    slabs, weight = call(
        functools.partial(slab_kernel, nr),
        (table, pixels, outside(weight), *halos),
        [pltpu.HBM((nc, groups * units, width), video.dtype), bf16(*weight.shape)],
        12,
        scratch=[
            VMEM((table.shape[1], width), video.dtype),
            VMEM((nc, groups * units, width), video.dtype),
            pltpu.SemaphoreType.DMA((nc + 1,)),
        ],
        hbm=(2,),
        out_hbm=(0,),
        flops=2 * table.size * width,
    )
    slabs = lax.all_to_all(slabs, "col", 0, 0, tiled=True)

    beside = swap(tokens, "col", 1)
    ring = [(i + d, i + 1 - d) for i in range(1, nc - 1, 2) for d in range(2)]
    edge = lax.ppermute(edge, "col", ring)

    held, others, offsets, bit = [tokens[None]], [beside[None]], [0], nc // 2
    while bit > 1:
        held.append(swap(joined(held), "col", bit))
        others.append(swap(held[-1], "col", 1))
        offsets += [o ^ bit for o in offsets]
        bit //= 2
    pieces = held + others

    keep, send, *rims = video_partials(weight, tokens, beside, edge, dims, channels)
    if nr == 2:
        rims = [swap(rims[0], "row", 1)]
    else:
        rims = [shift(rims[1], "row", 1), shift(rims[0], "row", -1)]
    keep, send = call(
        functools.partial(rim_kernel, (nm, nr)),
        (keep, send, *rims),
        [f32(*keep.shape), f32(*send.shape)],
        6,
    )
    video_grad = keep
    for s in range(1, nm):
        part = rotate(send[s - 1], "mp", s)
        video_grad = video_grad + part

    share = touched * KS
    out = call(
        functools.partial(weight_kernel, (groups, cols, units, share, len(pieces)), tuple(offsets)),
        (slabs, *pieces),
        [f32(share, half)] * nr,
        14,
        scratch=[
            VMEM((KS * units, groups * nc * cols), video.dtype),
            VMEM((half // 128, KS * units, 128), jnp.float32),
        ],
        flops=4 * units * KS * groups * nc * cols * half,
    )
    total = None
    for s, mine in enumerate(out):
        if block % KS:
            mine = lax.dynamic_slice_in_dim(mine, ((r + s) % nr * nc + c) * block % KS, block, 0)
        total = mine if s == 0 else total + rotate(mine, "row", s)
    weight_grad = total * lax.rsqrt(jnp.float32(count * nr * nc))
    return video_grad, weight_grad


def solution(mesh):
    return jax.shard_map(
        both_gradients,
        mesh=mesh,
        in_specs=(P(None, None, "row", "col"), P(None, "row", "col", "mp"), P(None, "mp")),
        out_specs=(P(None, "mp", "row", "col"), P(("row", "col"), "mp")),
        check_vma=False,
    )
```

```python
import functools

import jax
import jax.numpy as jnp
import numpy as np
from jax import lax
from jax.experimental import pallas as pl
from jax.experimental.pallas import tpu as pltpu
from jax.sharding import PartitionSpec as P

KT, KS, ST, SS = 4, 16, 2, 12
LAP = (KS - SS) // 2

VMEM = pltpu.VMEM


def grant(mib):
    return pltpu.CompilerParams(vmem_limit_bytes=mib << 20)


def swap(x, axis, bit):
    n = lax.axis_size(axis)
    return lax.ppermute(x, axis, [(i, i ^ bit) for i in range(n)])


def shift(x, axis, by):
    n = lax.axis_size(axis)
    return lax.ppermute(x, axis, [(i, i + by) for i in range(n) if 0 <= i + by < n])


def rotate(x, axis, by):
    n = lax.axis_size(axis)
    return lax.ppermute(x, axis, [(i, (i + by) % n) for i in range(n)])


def grid_of(rows, columns):
    return (
        lax.broadcasted_iota(jnp.int32, (rows, columns), 0),
        lax.broadcasted_iota(jnp.int32, (rows, columns), 1),
    )


def zero_one(mask):
    return jnp.where(mask, 1.0, 0.0).astype(jnp.bfloat16)


def fold_matrix(cols):
    n, x = grid_of(KS * cols, SS * cols)
    return zero_one(SS * lax.rem(n, cols) + lax.div(n, cols) - LAP == x)


def unfold_matrix(cols):
    width = SS * cols
    x, n = grid_of(width + 128, KS * cols)
    x = jnp.where(x < width + 64, x, x - width - 128)
    return zero_one(SS * lax.rem(n, cols) + lax.div(n, cols) - LAP == x)


def edge_rows(groups, cols, first):
    k, n = grid_of(16, groups * cols)
    firsts = (k >= groups) & (k < 2 * groups) & (n == (k - groups) * cols)
    lasts = (k < groups) & (n == k * cols + cols - 1)
    return zero_one(firsts & first | lasts & jnp.logical_not(first))


def lap_rows(images, height, lap, at):
    k, n = grid_of(lap, images * height)
    return zero_one((k < images * LAP) & (n == lax.div(k, LAP) * height + lax.rem(k, LAP) + at))


def row_tables(channels, frames, height, steps, rows, nr, nc, block, touched):
    inside, lap = channels * frames * height, halo_rows(channels, frames)
    m = np.zeros((nc, steps, rows, nr, touched, inside + 2 * lap), np.float32)
    for c, t, i, r, q in np.ndindex(*m.shape[:-1]):
        triple = (r * nc + c) * block // KS + q
        ch, a, b = triple // (KT * KS), triple // KS % KT, triple % KS
        f, y = ST * t + a - 1, SS * i + b - LAP
        if ch < channels and 0 <= f < frames:
            image = ch * frames + f
            if y < 0:
                k = inside + image * LAP + y + LAP
            elif y >= height:
                k = inside + lap + image * LAP + y - height
            else:
                k = image * height + y
            m[c, t, i, r, q, k] = 1
    m = m.reshape(nc, -1, m.shape[-1])
    used = m.any(-1)
    places = -(-used.sum(1).max() // 8) * 8
    table = np.zeros((nc, places, m.shape[-1]), np.float32)
    spread = np.zeros((nc, m.shape[1], places), np.float32)
    for c in range(nc):
        for place, row in enumerate(np.flatnonzero(used[c])):
            table[c, place] = m[c, row]
            spread[c, row, place] = 1
    return jnp.asarray(table, jnp.bfloat16), jnp.asarray(spread, jnp.bfloat16)


def halo_rows(channels, frames):
    return -(-channels * frames * LAP // 16) * 16


def exact(a, b):
    return jnp.dot(a, b, preferred_element_type=jnp.float32).astype(jnp.bfloat16)


def even_column():
    return lax.rem(lax.axis_index("col"), 2) == 0


def prep_kernel(dims, video_ref, flat_ref, table_ref, spread_ref, video_out, flat_out, table_out, spread_out, edge_ref, *refs):
    split, images, height, groups, cols = dims
    halos, sem = refs[:-1], refs[-1]
    spread = spread_ref.at[lax.axis_index("col")]
    pairs = ((flat_ref, flat_out), (video_ref, video_out), (table_ref, table_out), (spread, spread_out))
    moves = [pltpu.make_async_copy(a, b, sem.at[k]) for k, (a, b) in enumerate(pairs)]
    for move in moves:
        move.start()
    picked = edge_rows(groups, cols, even_column())
    lap = halos[0].shape[0]
    if split == 2:
        at = jnp.where(lax.axis_index("row") == 0, height - LAP, 0)
        rows = [lap_rows(images, height, lap, at)]
    else:
        rows = [lap_rows(images, height, lap, at) for at in (0, height - LAP)]
    moves[0].wait()
    edge_ref[...] = exact(picked, flat_out[...])
    moves[1].wait()
    for row, halo in zip(rows, halos):
        halo[...] = exact(row, video_out[...])
    moves[2].wait()
    moves[3].wait()


def slab_kernel(split, table_ref, video_ref, weight_ref, *refs):
    halos, out_ref, weight_out, v_ref, rows_ref, sem = refs[:-5], *refs[-5:]
    move = pltpu.make_async_copy(weight_ref.at[: weight_out.shape[0]], weight_out, sem.at[0])
    move.start()
    inside, lap = video_ref.shape[0], halos[0].shape[0]
    v_ref[:inside] = video_ref[...]
    if split == 2:
        row = lax.axis_index("row")
        halo = halos[0][...]
        zero = jnp.zeros_like(halo)
        v_ref[inside : inside + lap] = zero
        v_ref[inside + lap :] = zero

        @pl.when(row == 1)
        def _():
            v_ref[inside : inside + lap] = halo

        @pl.when(row == 0)
        def _():
            v_ref[inside + lap :] = halo
    else:
        v_ref[inside : inside + lap] = halos[0][...]
        v_ref[inside + lap :] = halos[1][...]
    moves = [move]
    for k in range(out_ref.shape[0]):
        rows_ref[k] = exact(table_ref[k], v_ref[...])
        moves.append(pltpu.make_async_copy(rows_ref.at[k], out_ref.at[k], sem.at[k + 1]))
        moves[-1].start()
    for move in moves:
        move.wait()


def video_kernel(dims, first_ref, w_ref, g_ref, beside_ref, edge_ref, *refs):
    steps, rows, cols, parts, split = dims
    keep_ref, send_ref = refs[:2]
    halos = refs[2:-5]
    p_ref, f_ref, t_ref, load_ref, sem = refs[-5:]
    count = steps * rows * cols
    channels, patch = p_ref.shape[0], p_ref.shape[2]
    moves = [
        pltpu.make_async_copy(w_ref.at[pl.ds(k * patch, patch)], load_ref.at[k - 1], sem.at[k - 1])
        for k in range(1, channels)
    ]
    for move in moves:
        move.start()
    picked = edge_rows(steps * rows, cols, even_column())
    t_ref[:count] = g_ref[...]
    t_ref[count:] = exact(picked, beside_ref[...]) + edge_ref[...]
    table = fold_matrix(cols)
    frames, _ = f_ref.shape[1:3]
    height, width = SS * rows, SS * cols
    entries = KT * KS
    tiles = count // 128
    lane = lax.broadcasted_iota(jnp.int32, (entries, 128), 1)
    f_ref[...] = jnp.zeros_like(f_ref)
    for ch in range(channels):
        if ch:
            moves[ch - 1].wait()
        p = lax.dot_general(
            first_ref[...] if ch == 0 else load_ref[ch - 1],
            t_ref[...],
            (((1,), (1,)), ((), ())),
            preferred_element_type=jnp.float32,
        )
        for k in range(tiles):
            p_ref[ch, k] = p[:, k * 128 : (k + 1) * 128]
        p_ref[ch, tiles, :, :16] = p[:, count:]
        strided = lambda k, e: p_ref.at[ch, k][pl.ds(e, entries, stride=KS), :]
        by_e = [[strided(k, e) for k in range(tiles)] for e in range(KS)]
        by_e = [jnp.concatenate(v, axis=1) if tiles > 1 else v[0] for v in by_e]
        groups = steps * rows
        left = [strided(tiles, KS - LAP + k) for k in range(LAP)]
        right = [strided(tiles, k) for k in range(LAP)]
        for t in range(steps):
            for i in range(rows):
                ti = t * rows + i
                edge = jnp.zeros((entries, 128), jnp.float32)
                for k in range(LAP):
                    for v, src, dst in ((left[k], ti, k), (right[k], groups + ti, 128 - LAP + k)):
                        v = v if src == dst else pltpu.roll(v, (dst - src) % 128, 1)
                        edge = jnp.where(lane == dst, v, edge)
                q = jnp.concatenate([v[:, ti * cols : (ti + 1) * cols] for v in by_e] + [edge], axis=1)
                for a in range(KT):
                    f = ST * t + a - 1
                    if 0 <= f < ST * steps:
                        top = 8 - LAP + SS * i
                        f_ref[ch, f, top : top + KS, :] += q[a * KS : (a + 1) * KS]
    per = frames // parts
    me = lax.axis_index("mp")
    depth = KS * cols

    def folded(v):
        high = v[:, :depth].astype(jnp.bfloat16)
        low = (v[:, :depth] - high.astype(jnp.float32)).astype(jnp.bfloat16)
        both = jnp.dot(jnp.concatenate([high, low], axis=0), table, preferred_element_type=jnp.float32)
        out = both[: v.shape[0]] + both[v.shape[0] :]
        edge = v[:, depth:]
        at = lax.broadcasted_iota(jnp.int32, edge.shape, 1)
        first = out[:, :128] + jnp.where(at < LAP, edge, 0.0)
        last = out[:, width - 128 :] + jnp.where(at >= 128 - LAP, edge, 0.0)
        return jnp.concatenate([first, out[:, 128 : width - 128], last], axis=1)

    inner = f_ref[:, :, 8 : 8 + height].reshape(channels * frames * height, depth + 128)
    inner = folded(inner).reshape(channels, frames, height, width)
    for g in range(parts):
        block = inner[:, g * per : (g + 1) * per]

        @pl.when(me == g)
        def _():
            keep_ref[...] = block

        for s in range(1, parts):

            @pl.when(lax.rem(me + s, parts) == g)
            def _():
                send_ref[s - 1] = block

    above = f_ref[:, :, 0:8].reshape(channels * frames * 8, depth + 128)
    below = f_ref[:, :, 8 + height : 16 + height].reshape(channels * frames * 8, depth + 128)
    unrolled = lambda v: folded(v).reshape(channels, frames, 8, width)
    if split == 2:
        up = lax.axis_index("row") != 0
        rim = unrolled(jnp.where(up, above, below))
        halos[0][...] = jnp.where(up, rim[:, :, 8 - LAP :], rim[:, :, :LAP])
    else:
        halos[0][...] = unrolled(above)[:, :, 8 - LAP :]
        halos[1][...] = unrolled(below)[:, :, :LAP]


def video_partials(first, weight, flat, beside, edge, dims, channels):
    steps, rows, cols, parts, split = dims
    half = weight.shape[1]
    patch = weight.shape[0] // channels
    frames = ST * steps
    per = frames // parts
    height, width = SS * rows, SS * cols
    sides = 1 if split == 2 else 2
    f32 = lambda *shape: jax.ShapeDtypeStruct(shape, jnp.float32)
    return call(
        functools.partial(video_kernel, dims),
        (first, outside(weight), flat, beside, edge),
        [f32(channels, per, height, width), f32(parts - 1, channels, per, height, width)]
        + [f32(channels, frames, LAP, width)] * sides,
        20,
        scratch=[
            VMEM((channels, flat.shape[0] // 128 + 1, patch, 128), jnp.float32),
            VMEM((channels, frames, height + 16, KS * cols + 128), jnp.float32),
            VMEM((flat.shape[0] + 16, half), flat.dtype),
            VMEM((channels - 1, patch, half), flat.dtype),
            pltpu.SemaphoreType.DMA((channels - 1,)),
        ],
        hbm=(1,),
        flops=4 * weight.size * flat.shape[0],
    )


def rim_kernel(dims, keep_ref, send_ref, *refs):
    parts, split = dims
    rims, (keep_out, send_out) = refs[:-2], refs[-2:]
    per, height = keep_ref.shape[1:3]
    me, row = lax.axis_index("mp"), lax.axis_index("row")
    for s in range(parts):
        src = keep_ref if s == 0 else send_ref.at[s - 1]
        out = keep_out if s == 0 else send_out.at[s - 1]
        out[...] = src[...]
        at = pl.ds(lax.rem(me + s, parts) * per, per)
        if split == 2:

            @pl.when(row == 1)
            def _():
                out[:, :, :LAP] += rims[0][:, at]

            @pl.when(row == 0)
            def _():
                out[:, :, height - LAP :] += rims[0][:, at]
        else:
            out[:, :, :LAP] += rims[0][:, at]
            out[:, :, height - LAP :] += rims[1][:, at]


def unfold_kernel(dims, offsets, slab_ref, spread_ref, a_ref):
    groups, cols, touched = dims
    nr, nc = lax.axis_size("row"), lax.axis_size("col")
    me = lax.axis_index("col")
    width = SS * cols
    places = slab_ref.shape[1]
    lane = lax.broadcasted_iota(jnp.int32, (places, 128), 1)
    order = [jnp.bitwise_xor(me, o + h) for h in range(2) for o in offsets]
    wide = []
    for c in order:
        mine = slab_ref[c]
        before = slab_ref[jnp.maximum(c - 1, 0)][:, width - 128 :].astype(jnp.float32)
        after = slab_ref[jnp.minimum(c + 1, nc - 1)][:, :128].astype(jnp.float32)
        mixed = jnp.where((lane >= 128 - LAP) & (c > 0), before, 0.0)
        mixed = jnp.where((lane < LAP) & (c < nc - 1), after, mixed)
        wide.append(jnp.concatenate([mine, mixed.astype(mine.dtype)], axis=1))
    flat = jnp.dot(jnp.concatenate(wide, axis=0), unfold_matrix(cols), preferred_element_type=jnp.float32)
    u = [
        jnp.dot(
            spread_ref[...],
            flat[k * places : (k + 1) * places].astype(jnp.bfloat16),
            preferred_element_type=jnp.float32,
        )
        for k in range(nc)
    ]
    pack = 128 // cols
    step = 2
    while step * touched % 16:
        step *= 2
    for cg in range(nc // pack):
        for e in range(0, KS, step):
            some = [
                jnp.concatenate(
                    [
                        u[cg * pack + c][:, (e + d) * cols : (e + d + 1) * cols]
                        for c in range(pack)
                    ],
                    axis=1,
                )
                for d in range(step)
            ]
            for ti in range(groups):
                lanes = slice(ti * nc * cols + cg * 128, ti * nc * cols + (cg + 1) * 128)
                for r in range(nr):
                    at = (ti * nr + r) * touched
                    both = jnp.concatenate([v[at : at + touched] for v in some], axis=0)
                    a_ref[r, e * touched : (e + step) * touched, lanes] = both.astype(a_ref.dtype)


def weight_kernel(dims, s, a_ref, *refs):
    groups, cols, touched = dims
    pieces, (out_ref, m_ref) = refs[:-2], refs[-2:]
    half = out_ref.shape[1]
    tokens = []
    for ti in range(groups):
        for ref in pieces:
            tokens.append(ref[:, ti * cols : (ti + 1) * cols, :].reshape(-1, half))
    owner = lax.rem(lax.axis_index("row") + s, lax.axis_size("row"))
    m = jnp.dot(a_ref[owner], jnp.concatenate(tokens, axis=0), preferred_element_type=jnp.float32)
    for k in range(m_ref.shape[0]):
        for e in range(KS):
            m_ref.at[k][pl.ds(e, touched, stride=KS), :] = m[e * touched : (e + 1) * touched, k * 128 : (k + 1) * 128]
        out_ref[:, k * 128 : (k + 1) * 128] = m_ref[k]


def joined(parts):
    return parts[0] if len(parts) == 1 else jnp.concatenate(parts, axis=0)


def outside(x):
    return pltpu.with_memory_space_constraint(x, pltpu.HBM)


def call(kernel, args, outs, mib, scratch=(), hbm=(), out_hbm=(), flops=1 << 20):
    space = lambda k, hbm: pltpu.HBM if k in hbm else VMEM
    return pl.pallas_call(
        kernel,
        in_specs=[pl.BlockSpec(memory_space=space(k, hbm)) for k in range(len(args))],
        out_specs=[pl.BlockSpec(memory_space=space(k, out_hbm)) for k in range(len(outs))],
        out_shape=outs,
        scratch_shapes=scratch,
        cost_estimate=pl.CostEstimate(flops=flops, bytes_accessed=1 << 20, transcendentals=0),
        compiler_params=grant(mib),
    )(*args)


def both_gradients(video, grad_tokens, weight):
    steps, rows, cols, half = grad_tokens.shape
    channels, frames, height, width = video.shape
    patch = weight.shape[0]
    nr, nc, nm = lax.axis_size("row"), lax.axis_size("col"), lax.axis_size("mp")
    r, c = lax.axis_index("row"), lax.axis_index("col")
    groups = steps * rows
    count = groups * cols
    flat = grad_tokens.reshape(count, half)
    pixels = video.reshape(-1, width)
    dims = (steps, rows, cols, nm, nr)
    images = channels * frames
    lap = halo_rows(channels, frames)
    block = patch // (nr * nc)
    touched = max((k * block % KS + block + KS - 1) // KS for k in range(nr * nc))
    units = nr * touched
    bf16 = lambda *shape: jax.ShapeDtypeStruct(shape, video.dtype)
    f32 = lambda *shape: jax.ShapeDtypeStruct(shape, jnp.float32)

    table, spread = row_tables(channels, frames, height, steps, rows, nr, nc, block, touched)
    places = table.shape[1]
    pixels, tokens, table, spread, edge, *halos = call(
        functools.partial(prep_kernel, (nr, images, height, groups, cols)),
        (outside(pixels), outside(flat), outside(table), outside(spread)),
        [bf16(*x.shape) for x in (pixels, flat, table)] + [bf16(*spread.shape[1:]), bf16(16, half)]
        + [bf16(lap, width)] * (1 if nr == 2 else 2),
        6,
        scratch=[pltpu.SemaphoreType.DMA((4,))],
        hbm=(0, 1, 2, 3),
    )
    if nr == 2:
        halos = [swap(halos[0], "row", 1)]
    else:
        halos = [shift(halos[1], "row", 1), shift(halos[0], "row", -1)]

    slabs, first = call(
        functools.partial(slab_kernel, nr),
        (table, pixels, outside(weight), *halos),
        [pltpu.HBM((nc, places, width), video.dtype), bf16(patch // channels, half)],
        12,
        scratch=[
            VMEM((table.shape[2], width), video.dtype),
            VMEM((nc, places, width), video.dtype),
            pltpu.SemaphoreType.DMA((nc + 1,)),
        ],
        hbm=(2,),
        out_hbm=(0,),
        flops=2 * table.size * width,
    )
    slabs = lax.all_to_all(slabs, "col", 0, 0, tiled=True)

    beside = swap(tokens, "col", 1)
    ring = [(i + d, i + 1 - d) for i in range(1, nc - 1, 2) for d in range(2)]
    edge = lax.ppermute(edge, "col", ring)

    held, offsets = [tokens[None]], [2 * k for k in range(nc // 2)]
    for bit in offsets[1:]:
        held.append(swap(tokens[None], "col", bit))
    others = [beside[None], swap(joined(held[1:]), "col", 1)]
    pieces = held + others

    keep, send, *rims = video_partials(first, weight, tokens, beside, edge, dims, channels)
    if nr == 2:
        rims = [swap(rims[0], "row", 1)]
    else:
        rims = [shift(rims[1], "row", 1), shift(rims[0], "row", -1)]
    keep, send = call(
        functools.partial(rim_kernel, (nm, nr)),
        (keep, send, *rims),
        [f32(*keep.shape), f32(*send.shape)],
        6,
    )
    video_grad = keep
    for s in range(1, nm):
        part = rotate(send[s - 1], "mp", s)
        video_grad = video_grad + part

    share = touched * KS
    (unfolded,) = call(
        functools.partial(unfold_kernel, (groups, cols, touched), tuple(offsets)),
        (slabs, spread),
        [bf16(nr, share, groups * nc * cols)],
        10,
        flops=2 * nc * groups * units * (width + 128) * KS * cols,
    )
    sums = [None] * nr
    for s in (*range(1, nr), 0):
        (mine,) = call(
            functools.partial(weight_kernel, (groups, cols, touched), s),
            (unfolded, *pieces),
            [f32(share, half)],
            8,
            scratch=[VMEM((half // 128, share, 128), jnp.float32)],
            flops=2 * share * groups * nc * cols * half,
        )
        if block % KS:
            mine = lax.dynamic_slice_in_dim(mine, ((r + s) % nr * nc + c) * block % KS, block, 0)
        sums[s] = rotate(mine, "row", s) if s else mine
    total = functools.reduce(jnp.add, sums)
    weight_grad = total * lax.rsqrt(jnp.float32(count * nr * nc))
    return video_grad, weight_grad


def solution(mesh):
    return jax.shard_map(
        both_gradients,
        mesh=mesh,
        in_specs=(P(None, None, "row", "col"), P(None, "row", "col", "mp"), P(None, "mp")),
        out_specs=(P(None, "mp", "row", "col"), P(("row", "col"), "mp")),
        check_vma=False,
    )
```

```python
import functools

import jax
import jax.numpy as jnp
import numpy as np
from jax import lax
from jax.experimental import pallas as pl
from jax.experimental.pallas import tpu as pltpu
from jax.sharding import PartitionSpec as P

KT, KS, ST, SS = 4, 16, 2, 12
LAP = (KS - SS) // 2

VMEM = pltpu.VMEM


def grant(mib):
    return pltpu.CompilerParams(vmem_limit_bytes=mib << 20)


def swap(x, axis, bit):
    n = lax.axis_size(axis)
    return lax.ppermute(x, axis, [(i, i ^ bit) for i in range(n)])


def shift(x, axis, by):
    n = lax.axis_size(axis)
    return lax.ppermute(x, axis, [(i, i + by) for i in range(n) if 0 <= i + by < n])


def rotate(x, axis, by):
    n = lax.axis_size(axis)
    return lax.ppermute(x, axis, [(i, (i + by) % n) for i in range(n)])


def grid_of(rows, columns):
    return (
        lax.broadcasted_iota(jnp.int32, (rows, columns), 0),
        lax.broadcasted_iota(jnp.int32, (rows, columns), 1),
    )


def zero_one(mask):
    return jnp.where(mask, 1.0, 0.0).astype(jnp.bfloat16)


def fold_matrix(cols):
    n, x = grid_of(KS * cols, SS * cols)
    return zero_one(SS * lax.rem(n, cols) + lax.div(n, cols) - LAP == x)


def unfold_matrix(cols):
    width = SS * cols
    x, n = grid_of(width + 128, KS * cols)
    x = jnp.where(x < width + 64, x, x - width - 128)
    return zero_one(SS * lax.rem(n, cols) + lax.div(n, cols) - LAP == x)


def edge_rows(groups, cols, first):
    k, n = grid_of(16, groups * cols)
    firsts = (k >= groups) & (k < 2 * groups) & (n == (k - groups) * cols)
    lasts = (k < groups) & (n == k * cols + cols - 1)
    return zero_one(firsts & first | lasts & jnp.logical_not(first))


def lap_rows(images, height, lap, at):
    k, n = grid_of(lap, images * height)
    return zero_one((k < images * LAP) & (n == lax.div(k, LAP) * height + lax.rem(k, LAP) + at))


def row_tables(channels, frames, height, steps, rows, nr, nc, block, touched):
    inside, lap = channels * frames * height, halo_rows(channels, frames)
    m = np.zeros((nc, steps, rows, nr, touched, inside + 2 * lap), np.float32)
    for c, t, i, r, q in np.ndindex(*m.shape[:-1]):
        triple = (r * nc + c) * block // KS + q
        ch, a, b = triple // (KT * KS), triple // KS % KT, triple % KS
        f, y = ST * t + a - 1, SS * i + b - LAP
        if ch < channels and 0 <= f < frames:
            image = ch * frames + f
            if y < 0:
                k = inside + image * LAP + y + LAP
            elif y >= height:
                k = inside + lap + image * LAP + y - height
            else:
                k = image * height + y
            m[c, t, i, r, q, k] = 1
    m = m.reshape(nc, -1, m.shape[-1])
    used = m.any(-1)
    places = -(-used.sum(1).max() // 8) * 8
    table = np.zeros((nc, places, m.shape[-1]), np.float32)
    spread = np.zeros((nc, m.shape[1], places), np.float32)
    for c in range(nc):
        for place, row in enumerate(np.flatnonzero(used[c])):
            table[c, place] = m[c, row]
            spread[c, row, place] = 1
    return jnp.asarray(table, jnp.bfloat16), jnp.asarray(spread, jnp.bfloat16)


def halo_rows(channels, frames):
    return -(-channels * frames * LAP // 16) * 16


def exact(a, b):
    return jnp.dot(a, b, preferred_element_type=jnp.float32).astype(jnp.bfloat16)


def even_column():
    return lax.rem(lax.axis_index("col"), 2) == 0


def prep_kernel(dims, video_ref, flat_ref, table_ref, spread_ref, video_out, flat_out, table_out, spread_out, edge_ref, *refs):
    split, images, height, groups, cols = dims
    halos, sem = refs[:-1], refs[-1]
    spread = spread_ref.at[lax.axis_index("col")]
    pairs = ((flat_ref, flat_out), (video_ref, video_out), (table_ref, table_out), (spread, spread_out))
    moves = [pltpu.make_async_copy(a, b, sem.at[k]) for k, (a, b) in enumerate(pairs)]
    for move in moves:
        move.start()
    picked = edge_rows(groups, cols, even_column())
    lap = halos[0].shape[0]
    if split == 2:
        at = jnp.where(lax.axis_index("row") == 0, height - LAP, 0)
        rows = [lap_rows(images, height, lap, at)]
    else:
        rows = [lap_rows(images, height, lap, at) for at in (0, height - LAP)]
    moves[0].wait()
    edge_ref[...] = exact(picked, flat_out[...])
    moves[1].wait()
    for row, halo in zip(rows, halos):
        halo[...] = exact(row, video_out[...])
    moves[2].wait()
    moves[3].wait()


def slab_kernel(split, table_ref, video_ref, weight_ref, *refs):
    halos, out_ref, weight_out, v_ref, rows_ref, sem = refs[:-5], *refs[-5:]
    move = pltpu.make_async_copy(weight_ref.at[: weight_out.shape[0]], weight_out, sem.at[0])
    move.start()
    inside, lap = video_ref.shape[0], halos[0].shape[0]
    v_ref[:inside] = video_ref[...]
    if split == 2:
        row = lax.axis_index("row")
        halo = halos[0][...]
        zero = jnp.zeros_like(halo)
        v_ref[inside : inside + lap] = zero
        v_ref[inside + lap :] = zero

        @pl.when(row == 1)
        def _():
            v_ref[inside : inside + lap] = halo

        @pl.when(row == 0)
        def _():
            v_ref[inside + lap :] = halo
    else:
        v_ref[inside : inside + lap] = halos[0][...]
        v_ref[inside + lap :] = halos[1][...]
    moves = [move]
    for k in range(out_ref.shape[0]):
        rows_ref[k] = exact(table_ref[k], v_ref[...])
        moves.append(pltpu.make_async_copy(rows_ref.at[k], out_ref.at[k], sem.at[k + 1]))
        moves[-1].start()
    for move in moves:
        move.wait()


def video_kernel(dims, first_ref, w_ref, g_ref, beside_ref, edge_ref, *refs):
    steps, rows, cols, parts, split = dims
    keep_ref, send_ref = refs[:2]
    halos = refs[2:-5]
    p_ref, f_ref, t_ref, load_ref, sem = refs[-5:]
    count = steps * rows * cols
    channels, patch = p_ref.shape[0], p_ref.shape[2]
    moves = [
        pltpu.make_async_copy(w_ref.at[pl.ds(k * patch, patch)], load_ref.at[k - 1], sem.at[k - 1])
        for k in range(1, channels)
    ]
    for move in moves:
        move.start()
    picked = edge_rows(steps * rows, cols, even_column())
    t_ref[:count] = g_ref[...]
    t_ref[count:] = exact(picked, beside_ref[0]) + edge_ref[...]
    table = fold_matrix(cols)
    frames, _ = f_ref.shape[1:3]
    height, width = SS * rows, SS * cols
    entries = KT * KS
    tiles = count // 128
    lane = lax.broadcasted_iota(jnp.int32, (entries, 128), 1)
    f_ref[...] = jnp.zeros_like(f_ref)
    for ch in range(channels):
        if ch:
            moves[ch - 1].wait()
        p = lax.dot_general(
            first_ref[...] if ch == 0 else load_ref[ch - 1],
            t_ref[...],
            (((1,), (1,)), ((), ())),
            preferred_element_type=jnp.float32,
        )
        for k in range(tiles):
            p_ref[ch, k] = p[:, k * 128 : (k + 1) * 128]
        p_ref[ch, tiles, :, :16] = p[:, count:]
        strided = lambda k, e: p_ref.at[ch, k][pl.ds(e, entries, stride=KS), :]
        by_e = [[strided(k, e) for k in range(tiles)] for e in range(KS)]
        by_e = [jnp.concatenate(v, axis=1) if tiles > 1 else v[0] for v in by_e]
        groups = steps * rows
        left = [strided(tiles, KS - LAP + k) for k in range(LAP)]
        right = [strided(tiles, k) for k in range(LAP)]
        for t in range(steps):
            for i in range(rows):
                ti = t * rows + i
                edge = jnp.zeros((entries, 128), jnp.float32)
                for k in range(LAP):
                    for v, src, dst in ((left[k], ti, k), (right[k], groups + ti, 128 - LAP + k)):
                        v = v if src == dst else pltpu.roll(v, (dst - src) % 128, 1)
                        edge = jnp.where(lane == dst, v, edge)
                q = jnp.concatenate([v[:, ti * cols : (ti + 1) * cols] for v in by_e] + [edge], axis=1)
                for a in range(KT):
                    f = ST * t + a - 1
                    if 0 <= f < ST * steps:
                        top = 8 - LAP + SS * i
                        f_ref[ch, f, top : top + KS, :] += q[a * KS : (a + 1) * KS]
    per = frames // parts
    me = lax.axis_index("mp")
    depth = KS * cols

    def folded(v):
        high = v[:, :depth].astype(jnp.bfloat16)
        low = (v[:, :depth] - high.astype(jnp.float32)).astype(jnp.bfloat16)
        both = jnp.dot(jnp.concatenate([high, low], axis=0), table, preferred_element_type=jnp.float32)
        out = both[: v.shape[0]] + both[v.shape[0] :]
        edge = v[:, depth:]
        at = lax.broadcasted_iota(jnp.int32, edge.shape, 1)
        first = out[:, :128] + jnp.where(at < LAP, edge, 0.0)
        last = out[:, width - 128 :] + jnp.where(at >= 128 - LAP, edge, 0.0)
        return jnp.concatenate([first, out[:, 128 : width - 128], last], axis=1)

    inner = f_ref[:, :, 8 : 8 + height].reshape(channels * frames * height, depth + 128)
    inner = folded(inner).reshape(channels, frames, height, width)
    for g in range(parts):
        block = inner[:, g * per : (g + 1) * per]

        @pl.when(me == g)
        def _():
            keep_ref[...] = block

        for s in range(1, parts):

            @pl.when(lax.rem(me + s, parts) == g)
            def _():
                send_ref[s - 1] = block

    above = f_ref[:, :, 0:8].reshape(channels * frames * 8, depth + 128)
    below = f_ref[:, :, 8 + height : 16 + height].reshape(channels * frames * 8, depth + 128)
    unrolled = lambda v: folded(v).reshape(channels, frames, 8, width)
    if split == 2:
        up = lax.axis_index("row") != 0
        rim = unrolled(jnp.where(up, above, below))
        halos[0][...] = jnp.where(up, rim[:, :, 8 - LAP :], rim[:, :, :LAP])
    else:
        halos[0][...] = unrolled(above)[:, :, 8 - LAP :]
        halos[1][...] = unrolled(below)[:, :, :LAP]


def video_partials(first, weight, flat, beside, edge, dims, channels):
    steps, rows, cols, parts, split = dims
    half = weight.shape[1]
    patch = weight.shape[0] // channels
    frames = ST * steps
    per = frames // parts
    height, width = SS * rows, SS * cols
    sides = 1 if split == 2 else 2
    f32 = lambda *shape: jax.ShapeDtypeStruct(shape, jnp.float32)
    return call(
        functools.partial(video_kernel, dims),
        (first, outside(weight), flat, beside, edge),
        [f32(channels, per, height, width), f32(parts - 1, channels, per, height, width)]
        + [f32(channels, frames, LAP, width)] * sides,
        20,
        scratch=[
            VMEM((channels, flat.shape[0] // 128 + 1, patch, 128), jnp.float32),
            VMEM((channels, frames, height + 16, KS * cols + 128), jnp.float32),
            VMEM((flat.shape[0] + 16, half), flat.dtype),
            VMEM((channels - 1, patch, half), flat.dtype),
            pltpu.SemaphoreType.DMA((channels - 1,)),
        ],
        hbm=(1,),
        flops=4 * weight.size * flat.shape[0],
    )


def rim_kernel(dims, keep_ref, send_ref, *refs):
    parts, split = dims
    rims, (keep_out, send_out) = refs[:-2], refs[-2:]
    per, height = keep_ref.shape[1:3]
    me, row = lax.axis_index("mp"), lax.axis_index("row")
    for s in range(parts):
        src = keep_ref if s == 0 else send_ref.at[s - 1]
        out = keep_out if s == 0 else send_out.at[s - 1]
        out[...] = src[...]
        at = pl.ds(lax.rem(me + s, parts) * per, per)
        if split == 2:

            @pl.when(row == 1)
            def _():
                out[:, :, :LAP] += rims[0][:, at]

            @pl.when(row == 0)
            def _():
                out[:, :, height - LAP :] += rims[0][:, at]
        else:
            out[:, :, :LAP] += rims[0][:, at]
            out[:, :, height - LAP :] += rims[1][:, at]


def unfold_kernel(dims, offsets, slab_ref, spread_ref, a_ref):
    groups, cols, touched = dims
    nr, nc = lax.axis_size("row"), lax.axis_size("col")
    me = lax.axis_index("col")
    width = SS * cols
    places = slab_ref.shape[1]
    lane = lax.broadcasted_iota(jnp.int32, (places, 128), 1)
    order = [jnp.bitwise_xor(me, o + h) for h in range(2) for o in offsets]
    wide = []
    for c in order:
        mine = slab_ref[c]
        before = slab_ref[jnp.maximum(c - 1, 0)][:, width - 128 :].astype(jnp.float32)
        after = slab_ref[jnp.minimum(c + 1, nc - 1)][:, :128].astype(jnp.float32)
        mixed = jnp.where((lane >= 128 - LAP) & (c > 0), before, 0.0)
        mixed = jnp.where((lane < LAP) & (c < nc - 1), after, mixed)
        wide.append(jnp.concatenate([mine, mixed.astype(mine.dtype)], axis=1))
    flat = jnp.dot(jnp.concatenate(wide, axis=0), unfold_matrix(cols), preferred_element_type=jnp.float32)
    u = [
        jnp.dot(
            spread_ref[...],
            flat[k * places : (k + 1) * places].astype(jnp.bfloat16),
            preferred_element_type=jnp.float32,
        )
        for k in range(nc)
    ]
    pack = 128 // cols
    step = 2
    while step * touched % 16:
        step *= 2
    for cg in range(nc // pack):
        for e in range(0, KS, step):
            some = [
                jnp.concatenate(
                    [
                        u[cg * pack + c][:, (e + d) * cols : (e + d + 1) * cols]
                        for c in range(pack)
                    ],
                    axis=1,
                )
                for d in range(step)
            ]
            for ti in range(groups):
                lanes = slice(ti * nc * cols + cg * 128, ti * nc * cols + (cg + 1) * 128)
                for r in range(nr):
                    at = (ti * nr + r) * touched
                    both = jnp.concatenate([v[at : at + touched] for v in some], axis=0)
                    a_ref[r, e * touched : (e + step) * touched, lanes] = both.astype(a_ref.dtype)


def weight_kernel(dims, s, a_ref, *refs):
    groups, cols, touched = dims
    pieces, (out_ref, m_ref) = refs[:-2], refs[-2:]
    half = out_ref.shape[1]
    tokens = []
    for ti in range(groups):
        for ref in pieces:
            tokens.append(ref[:, ti * cols : (ti + 1) * cols, :].reshape(-1, half))
    owner = lax.rem(lax.axis_index("row") + s, lax.axis_size("row"))
    m = jnp.dot(a_ref[owner], jnp.concatenate(tokens, axis=0), preferred_element_type=jnp.float32)
    for k in range(m_ref.shape[0]):
        for e in range(KS):
            m_ref.at[k][pl.ds(e, touched, stride=KS), :] = m[e * touched : (e + 1) * touched, k * 128 : (k + 1) * 128]
        out_ref[:, k * 128 : (k + 1) * 128] = m_ref[k]


def joined(parts):
    return parts[0] if len(parts) == 1 else jnp.concatenate(parts, axis=0)


def outside(x):
    return pltpu.with_memory_space_constraint(x, pltpu.HBM)


def call(kernel, args, outs, mib, scratch=(), hbm=(), out_hbm=(), flops=1 << 20):
    space = lambda k, hbm: pltpu.HBM if k in hbm else VMEM
    return pl.pallas_call(
        kernel,
        in_specs=[pl.BlockSpec(memory_space=space(k, hbm)) for k in range(len(args))],
        out_specs=[pl.BlockSpec(memory_space=space(k, out_hbm)) for k in range(len(outs))],
        out_shape=outs,
        scratch_shapes=scratch,
        cost_estimate=pl.CostEstimate(flops=flops, bytes_accessed=1 << 20, transcendentals=0),
        compiler_params=grant(mib),
    )(*args)


def both_gradients(video, grad_tokens, weight):
    steps, rows, cols, half = grad_tokens.shape
    channels, frames, height, width = video.shape
    patch = weight.shape[0]
    nr, nc, nm = lax.axis_size("row"), lax.axis_size("col"), lax.axis_size("mp")
    r, c = lax.axis_index("row"), lax.axis_index("col")
    groups = steps * rows
    count = groups * cols
    flat = grad_tokens.reshape(count, half)
    pixels = video.reshape(-1, width)
    dims = (steps, rows, cols, nm, nr)
    images = channels * frames
    lap = halo_rows(channels, frames)
    block = patch // (nr * nc)
    touched = max((k * block % KS + block + KS - 1) // KS for k in range(nr * nc))
    units = nr * touched
    bf16 = lambda *shape: jax.ShapeDtypeStruct(shape, video.dtype)
    f32 = lambda *shape: jax.ShapeDtypeStruct(shape, jnp.float32)

    table, spread = row_tables(channels, frames, height, steps, rows, nr, nc, block, touched)
    places = table.shape[1]
    pixels, tokens, table, spread, edge, *halos = call(
        functools.partial(prep_kernel, (nr, images, height, groups, cols)),
        (outside(pixels), outside(flat), outside(table), outside(spread)),
        [bf16(*x.shape) for x in (pixels, flat, table)] + [bf16(*spread.shape[1:]), bf16(16, half)]
        + [bf16(lap, width)] * (1 if nr == 2 else 2),
        6,
        scratch=[pltpu.SemaphoreType.DMA((4,))],
        hbm=(0, 1, 2, 3),
    )
    if nr == 2:
        halos = [swap(halos[0], "row", 1)]
    else:
        halos = [shift(halos[1], "row", 1), shift(halos[0], "row", -1)]

    slabs, first = call(
        functools.partial(slab_kernel, nr),
        (table, pixels, outside(weight), *halos),
        [pltpu.HBM((nc, places, width), video.dtype), bf16(patch // channels, half)],
        12,
        scratch=[
            VMEM((table.shape[2], width), video.dtype),
            VMEM((nc, places, width), video.dtype),
            pltpu.SemaphoreType.DMA((nc + 1,)),
        ],
        hbm=(2,),
        out_hbm=(0,),
        flops=2 * table.size * width,
    )
    slabs = lax.all_to_all(slabs, "col", 0, 0, tiled=True)

    ring = [(i + d, i + 1 - d) for i in range(1, nc - 1, 2) for d in range(2)]
    edge = lax.ppermute(edge, "col", ring)
    held, offsets = [tokens[None]], [2 * k for k in range(nc // 2)]
    for bit in offsets[1:]:
        held.append(swap(tokens[None], "col", bit))
    beside = swap(joined(held[:2]), "col", 1)
    others = [beside, swap(joined(held[2:]), "col", 1)]
    pieces = held + others

    keep, send, *rims = video_partials(first, weight, tokens, beside, edge, dims, channels)
    if nr == 2:
        rims = [swap(rims[0], "row", 1)]
    else:
        rims = [shift(rims[1], "row", 1), shift(rims[0], "row", -1)]
    keep, send = call(
        functools.partial(rim_kernel, (nm, nr)),
        (keep, send, *rims),
        [f32(*keep.shape), f32(*send.shape)],
        6,
    )
    video_grad = keep
    for s in range(1, nm):
        part = rotate(send[s - 1], "mp", s)
        video_grad = video_grad + part

    share = touched * KS
    (unfolded,) = call(
        functools.partial(unfold_kernel, (groups, cols, touched), tuple(offsets)),
        (slabs, spread),
        [bf16(nr, share, groups * nc * cols)],
        10,
        flops=2 * nc * groups * units * (width + 128) * KS * cols,
    )
    sums = [None] * nr
    for s in (*range(1, nr), 0):
        (mine,) = call(
            functools.partial(weight_kernel, (groups, cols, touched), s),
            (unfolded, *pieces),
            [f32(share, half)],
            8,
            scratch=[VMEM((half // 128, share, 128), jnp.float32)],
            flops=2 * share * groups * nc * cols * half,
        )
        if block % KS:
            mine = lax.dynamic_slice_in_dim(mine, ((r + s) % nr * nc + c) * block % KS, block, 0)
        sums[s] = rotate(mine, "row", s) if s else mine
    total = functools.reduce(jnp.add, sums)
    weight_grad = total * lax.rsqrt(jnp.float32(count * nr * nc))
    return video_grad, weight_grad


def solution(mesh):
    return jax.shard_map(
        both_gradients,
        mesh=mesh,
        in_specs=(P(None, None, "row", "col"), P(None, "row", "col", "mp"), P(None, "mp")),
        out_specs=(P(None, "mp", "row", "col"), P(("row", "col"), "mp")),
        check_vma=False,
    )
```

```python
import functools

import jax
import jax.numpy as jnp
import numpy as np
from jax import lax
from jax.experimental import pallas as pl
from jax.experimental.pallas import tpu as pltpu
from jax.sharding import PartitionSpec as P

KT, KS, ST, SS = 4, 16, 2, 12
LAP = (KS - SS) // 2

VMEM = pltpu.VMEM


def grant(mib):
    return pltpu.CompilerParams(vmem_limit_bytes=mib << 20)


def swap(x, axis, bit):
    n = lax.axis_size(axis)
    return lax.ppermute(x, axis, [(i, i ^ bit) for i in range(n)])


def shift(x, axis, by):
    n = lax.axis_size(axis)
    return lax.ppermute(x, axis, [(i, i + by) for i in range(n) if 0 <= i + by < n])


def rotate(x, axis, by):
    n = lax.axis_size(axis)
    return lax.ppermute(x, axis, [(i, (i + by) % n) for i in range(n)])


def grid_of(rows, columns):
    return (
        lax.broadcasted_iota(jnp.int32, (rows, columns), 0),
        lax.broadcasted_iota(jnp.int32, (rows, columns), 1),
    )


def zero_one(mask):
    return jnp.where(mask, 1.0, 0.0).astype(jnp.bfloat16)


def fold_matrix(cols):
    n, x = grid_of(KS * cols, SS * cols)
    return zero_one(SS * lax.rem(n, cols) + lax.div(n, cols) - LAP == x)


def unfold_matrix(cols):
    width = SS * cols
    x, n = grid_of(width + 128, KS * cols)
    x = jnp.where(x < width + 64, x, x - width - 128)
    return zero_one(SS * lax.rem(n, cols) + lax.div(n, cols) - LAP == x)


def edge_rows(groups, cols, first):
    k, n = grid_of(16, groups * cols)
    firsts = (k >= groups) & (k < 2 * groups) & (n == (k - groups) * cols)
    lasts = (k < groups) & (n == k * cols + cols - 1)
    return zero_one(firsts & first | lasts & jnp.logical_not(first))


def lap_rows(images, height, lap, at):
    k, n = grid_of(lap, images * height)
    return zero_one((k < images * LAP) & (n == lax.div(k, LAP) * height + lax.rem(k, LAP) + at))


def row_tables(channels, frames, height, steps, rows, nr, nc, block, touched):
    inside, lap = channels * frames * height, halo_rows(channels, frames)
    m = np.zeros((nc, steps, rows, nr, touched, inside + 2 * lap), np.float32)
    for c, t, i, r, q in np.ndindex(*m.shape[:-1]):
        triple = (r * nc + c) * block // KS + q
        ch, a, b = triple // (KT * KS), triple // KS % KT, triple % KS
        f, y = ST * t + a - 1, SS * i + b - LAP
        if ch < channels and 0 <= f < frames:
            image = ch * frames + f
            if y < 0:
                k = inside + image * LAP + y + LAP
            elif y >= height:
                k = inside + lap + image * LAP + y - height
            else:
                k = image * height + y
            m[c, t, i, r, q, k] = 1
    m = m.reshape(nc, -1, m.shape[-1])
    used = m.any(-1)
    places = -(-used.sum(1).max() // 8) * 8
    table = np.zeros((nc, places, m.shape[-1]), np.float32)
    spread = np.zeros((nc, m.shape[1], places), np.float32)
    for c in range(nc):
        for place, row in enumerate(np.flatnonzero(used[c])):
            table[c, place] = m[c, row]
            spread[c, row, place] = 1
    return jnp.asarray(table, jnp.bfloat16), jnp.asarray(spread, jnp.bfloat16)


def halo_rows(channels, frames):
    return -(-channels * frames * LAP // 16) * 16


def exact(a, b):
    return jnp.dot(a, b, preferred_element_type=jnp.float32).astype(jnp.bfloat16)


def even_column():
    return lax.rem(lax.axis_index("col"), 2) == 0


def prep_kernel(dims, video_ref, flat_ref, table_ref, spread_ref, video_out, flat_out, table_out, spread_out, edge_ref, *refs):
    split, images, height, groups, cols = dims
    halos, sem = refs[:-1], refs[-1]
    spread = spread_ref.at[lax.axis_index("col")]
    pairs = ((flat_ref, flat_out), (video_ref, video_out), (table_ref, table_out), (spread, spread_out))
    moves = [pltpu.make_async_copy(a, b, sem.at[k]) for k, (a, b) in enumerate(pairs)]
    for move in moves:
        move.start()
    picked = edge_rows(groups, cols, even_column())
    lap = halos[0].shape[0]
    if split == 2:
        at = jnp.where(lax.axis_index("row") == 0, height - LAP, 0)
        rows = [lap_rows(images, height, lap, at)]
    else:
        rows = [lap_rows(images, height, lap, at) for at in (0, height - LAP)]
    moves[0].wait()
    edge_ref[...] = exact(picked, flat_out[...])
    moves[1].wait()
    for row, halo in zip(rows, halos):
        halo[...] = exact(row, video_out[...])
    moves[2].wait()
    moves[3].wait()


def slab_kernel(split, table_ref, video_ref, weight_ref, *refs):
    halos, out_ref, weight_out, v_ref, rows_ref, sem = refs[:-5], *refs[-5:]
    move = pltpu.make_async_copy(weight_ref.at[: weight_out.shape[0]], weight_out, sem.at[0])
    move.start()
    inside, lap = video_ref.shape[0], halos[0].shape[0]
    v_ref[:inside] = video_ref[...]
    if split == 2:
        row = lax.axis_index("row")
        halo = halos[0][...]
        zero = jnp.zeros_like(halo)
        v_ref[inside : inside + lap] = zero
        v_ref[inside + lap :] = zero

        @pl.when(row == 1)
        def _():
            v_ref[inside : inside + lap] = halo

        @pl.when(row == 0)
        def _():
            v_ref[inside + lap :] = halo
    else:
        v_ref[inside : inside + lap] = halos[0][...]
        v_ref[inside + lap :] = halos[1][...]
    moves = [move]
    for k in range(out_ref.shape[0]):
        rows_ref[k] = exact(table_ref[k], v_ref[...])
        moves.append(pltpu.make_async_copy(rows_ref.at[k], out_ref.at[k], sem.at[k + 1]))
        moves[-1].start()
    for move in moves:
        move.wait()


def video_kernel(dims, first_ref, w_ref, g_ref, beside_ref, edge_ref, *refs):
    steps, rows, cols, parts, split = dims
    keep_ref, send_ref = refs[:2]
    halos = refs[2:-5]
    p_ref, f_ref, t_ref, load_ref, sem = refs[-5:]
    count = steps * rows * cols
    channels, patch = p_ref.shape[0], p_ref.shape[2]
    moves = [
        pltpu.make_async_copy(w_ref.at[pl.ds(k * patch, patch)], load_ref.at[k - 1], sem.at[k - 1])
        for k in range(1, channels)
    ]
    for move in moves:
        move.start()
    picked = edge_rows(steps * rows, cols, even_column())
    t_ref[:count] = g_ref[...]
    t_ref[count:] = exact(picked, beside_ref[0]) + edge_ref[...]
    table = fold_matrix(cols)
    frames, _ = f_ref.shape[1:3]
    height, width = SS * rows, SS * cols
    entries = KT * KS
    tiles = count // 128
    lane = lax.broadcasted_iota(jnp.int32, (entries, 128), 1)
    f_ref[...] = jnp.zeros_like(f_ref)
    for ch in range(channels):
        if ch:
            moves[ch - 1].wait()
        p = lax.dot_general(
            first_ref[...] if ch == 0 else load_ref[ch - 1],
            t_ref[...],
            (((1,), (1,)), ((), ())),
            preferred_element_type=jnp.float32,
        )
        for k in range(tiles):
            p_ref[ch, k] = p[:, k * 128 : (k + 1) * 128]
        p_ref[ch, tiles, :, :16] = p[:, count:]
        strided = lambda k, e: p_ref.at[ch, k][pl.ds(e, entries, stride=KS), :]
        by_e = [[strided(k, e) for k in range(tiles)] for e in range(KS)]
        by_e = [jnp.concatenate(v, axis=1) if tiles > 1 else v[0] for v in by_e]
        groups = steps * rows
        left = [strided(tiles, KS - LAP + k) for k in range(LAP)]
        right = [strided(tiles, k) for k in range(LAP)]
        for t in range(steps):
            for i in range(rows):
                ti = t * rows + i
                edge = jnp.zeros((entries, 128), jnp.float32)
                for k in range(LAP):
                    for v, src, dst in ((left[k], ti, k), (right[k], groups + ti, 128 - LAP + k)):
                        v = v if src == dst else pltpu.roll(v, (dst - src) % 128, 1)
                        edge = jnp.where(lane == dst, v, edge)
                q = jnp.concatenate([v[:, ti * cols : (ti + 1) * cols] for v in by_e] + [edge], axis=1)
                for a in range(KT):
                    f = ST * t + a - 1
                    if 0 <= f < ST * steps:
                        top = 8 - LAP + SS * i
                        f_ref[ch, f, top : top + KS, :] += q[a * KS : (a + 1) * KS]
    per = frames // parts
    me = lax.axis_index("mp")
    depth = KS * cols

    def folded(v):
        high = v[:, :depth].astype(jnp.bfloat16)
        low = (v[:, :depth] - high.astype(jnp.float32)).astype(jnp.bfloat16)
        both = jnp.dot(jnp.concatenate([high, low], axis=0), table, preferred_element_type=jnp.float32)
        out = both[: v.shape[0]] + both[v.shape[0] :]
        edge = v[:, depth:]
        at = lax.broadcasted_iota(jnp.int32, edge.shape, 1)
        first = out[:, :128] + jnp.where(at < LAP, edge, 0.0)
        last = out[:, width - 128 :] + jnp.where(at >= 128 - LAP, edge, 0.0)
        return jnp.concatenate([first, out[:, 128 : width - 128], last], axis=1)

    inner = f_ref[:, :, 8 : 8 + height].reshape(channels * frames * height, depth + 128)
    inner = folded(inner).reshape(channels, frames, height, width)
    for g in range(parts):
        block = inner[:, g * per : (g + 1) * per]

        @pl.when(me == g)
        def _():
            keep_ref[...] = block

        for s in range(1, parts):

            @pl.when(lax.rem(me + s, parts) == g)
            def _():
                send_ref[s - 1] = block

    above = f_ref[:, :, 0:8].reshape(channels * frames * 8, depth + 128)
    below = f_ref[:, :, 8 + height : 16 + height].reshape(channels * frames * 8, depth + 128)
    unrolled = lambda v: folded(v).reshape(channels, frames, 8, width)
    if split == 2:
        up = lax.axis_index("row") != 0
        rim = unrolled(jnp.where(up, above, below))
        halos[0][...] = jnp.where(up, rim[:, :, 8 - LAP :], rim[:, :, :LAP])
    else:
        halos[0][...] = unrolled(above)[:, :, 8 - LAP :]
        halos[1][...] = unrolled(below)[:, :, :LAP]


def video_partials(first, weight, flat, beside, edge, dims, channels):
    steps, rows, cols, parts, split = dims
    half = weight.shape[1]
    patch = weight.shape[0] // channels
    frames = ST * steps
    per = frames // parts
    height, width = SS * rows, SS * cols
    sides = 1 if split == 2 else 2
    f32 = lambda *shape: jax.ShapeDtypeStruct(shape, jnp.float32)
    return call(
        functools.partial(video_kernel, dims),
        (first, outside(weight), flat, beside, edge),
        [f32(channels, per, height, width), f32(parts - 1, channels, per, height, width)]
        + [f32(channels, frames, LAP, width)] * sides,
        20,
        scratch=[
            VMEM((channels, flat.shape[0] // 128 + 1, patch, 128), jnp.float32),
            VMEM((channels, frames, height + 16, KS * cols + 128), jnp.float32),
            VMEM((flat.shape[0] + 16, half), flat.dtype),
            VMEM((channels - 1, patch, half), flat.dtype),
            pltpu.SemaphoreType.DMA((channels - 1,)),
        ],
        hbm=(1,),
        flops=4 * weight.size * flat.shape[0],
    )


def rim_kernel(dims, keep_ref, send_ref, *refs):
    parts, split = dims
    rims, (keep_out, send_out) = refs[:-2], refs[-2:]
    per, height = keep_ref.shape[1:3]
    me, row = lax.axis_index("mp"), lax.axis_index("row")
    for s in range(parts):
        src = keep_ref if s == 0 else send_ref.at[s - 1]
        out = keep_out if s == 0 else send_out.at[s - 1]
        out[...] = src[...]
        at = pl.ds(lax.rem(me + s, parts) * per, per)
        if split == 2:

            @pl.when(row == 1)
            def _():
                out[:, :, :LAP] += rims[0][:, at]

            @pl.when(row == 0)
            def _():
                out[:, :, height - LAP :] += rims[0][:, at]
        else:
            out[:, :, :LAP] += rims[0][:, at]
            out[:, :, height - LAP :] += rims[1][:, at]


def table_kernel(cols, out_ref):
    out_ref[...] = unfold_matrix(cols)


def unfold_kernel(dims, offsets, slab_ref, spread_ref, table_ref, a_ref):
    groups, cols, touched = dims
    nr, nc = lax.axis_size("row"), lax.axis_size("col")
    me = lax.axis_index("col")
    width = SS * cols
    places = slab_ref.shape[1]
    lane = lax.broadcasted_iota(jnp.int32, (places, 128), 1)
    order = [jnp.bitwise_xor(me, o + h) for h in range(2) for o in offsets]
    wide = []
    for c in order:
        mine = slab_ref[c]
        before = slab_ref[jnp.maximum(c - 1, 0)][:, width - 128 :].astype(jnp.float32)
        after = slab_ref[jnp.minimum(c + 1, nc - 1)][:, :128].astype(jnp.float32)
        mixed = jnp.where((lane >= 128 - LAP) & (c > 0), before, 0.0)
        mixed = jnp.where((lane < LAP) & (c < nc - 1), after, mixed)
        wide.append(jnp.concatenate([mine, mixed.astype(mine.dtype)], axis=1))
    flat = jnp.dot(jnp.concatenate(wide, axis=0), table_ref[...], preferred_element_type=jnp.float32)
    u = [
        jnp.dot(
            spread_ref[...],
            flat[k * places : (k + 1) * places].astype(jnp.bfloat16),
            preferred_element_type=jnp.float32,
        )
        for k in range(nc)
    ]
    pack = 128 // cols
    step = 2
    while step * touched % 16:
        step *= 2
    for cg in range(nc // pack):
        for e in range(0, KS, step):
            some = [
                jnp.concatenate(
                    [
                        u[cg * pack + c][:, (e + d) * cols : (e + d + 1) * cols]
                        for c in range(pack)
                    ],
                    axis=1,
                )
                for d in range(step)
            ]
            for ti in range(groups):
                lanes = slice(ti * nc * cols + cg * 128, ti * nc * cols + (cg + 1) * 128)
                for r in range(nr):
                    at = (ti * nr + r) * touched
                    both = jnp.concatenate([v[at : at + touched] for v in some], axis=0)
                    a_ref[r, e * touched : (e + step) * touched, lanes] = both.astype(a_ref.dtype)


def weight_kernel(dims, s, a_ref, *refs):
    groups, cols, touched = dims
    pieces, (out_ref, m_ref) = refs[:-2], refs[-2:]
    half = out_ref.shape[1]
    tokens = []
    for ti in range(groups):
        for ref in pieces:
            tokens.append(ref[:, ti * cols : (ti + 1) * cols, :].reshape(-1, half))
    owner = lax.rem(lax.axis_index("row") + s, lax.axis_size("row"))
    m = jnp.dot(a_ref[owner], jnp.concatenate(tokens, axis=0), preferred_element_type=jnp.float32)
    for k in range(m_ref.shape[0]):
        for e in range(KS):
            m_ref.at[k][pl.ds(e, touched, stride=KS), :] = m[e * touched : (e + 1) * touched, k * 128 : (k + 1) * 128]
        out_ref[:, k * 128 : (k + 1) * 128] = m_ref[k]


def joined(parts):
    return parts[0] if len(parts) == 1 else jnp.concatenate(parts, axis=0)


def outside(x):
    return pltpu.with_memory_space_constraint(x, pltpu.HBM)


def call(kernel, args, outs, mib, scratch=(), hbm=(), out_hbm=(), flops=1 << 20):
    space = lambda k, hbm: pltpu.HBM if k in hbm else VMEM
    return pl.pallas_call(
        kernel,
        in_specs=[pl.BlockSpec(memory_space=space(k, hbm)) for k in range(len(args))],
        out_specs=[pl.BlockSpec(memory_space=space(k, out_hbm)) for k in range(len(outs))],
        out_shape=outs,
        scratch_shapes=scratch,
        cost_estimate=pl.CostEstimate(flops=flops, bytes_accessed=1 << 20, transcendentals=0),
        compiler_params=grant(mib),
    )(*args)


def both_gradients(video, grad_tokens, weight):
    steps, rows, cols, half = grad_tokens.shape
    channels, frames, height, width = video.shape
    patch = weight.shape[0]
    nr, nc, nm = lax.axis_size("row"), lax.axis_size("col"), lax.axis_size("mp")
    r, c = lax.axis_index("row"), lax.axis_index("col")
    groups = steps * rows
    count = groups * cols
    flat = grad_tokens.reshape(count, half)
    pixels = video.reshape(-1, width)
    dims = (steps, rows, cols, nm, nr)
    images = channels * frames
    lap = halo_rows(channels, frames)
    block = patch // (nr * nc)
    touched = max((k * block % KS + block + KS - 1) // KS for k in range(nr * nc))
    units = nr * touched
    bf16 = lambda *shape: jax.ShapeDtypeStruct(shape, video.dtype)
    f32 = lambda *shape: jax.ShapeDtypeStruct(shape, jnp.float32)

    table, spread = row_tables(channels, frames, height, steps, rows, nr, nc, block, touched)
    places = table.shape[1]
    pixels, tokens, table, spread, edge, *halos = call(
        functools.partial(prep_kernel, (nr, images, height, groups, cols)),
        (outside(pixels), outside(flat), outside(table), outside(spread)),
        [bf16(*x.shape) for x in (pixels, flat, table)] + [bf16(*spread.shape[1:]), bf16(16, half)]
        + [bf16(lap, width)] * (1 if nr == 2 else 2),
        6,
        scratch=[pltpu.SemaphoreType.DMA((4,))],
        hbm=(0, 1, 2, 3),
    )
    if nr == 2:
        halos = [swap(halos[0], "row", 1)]
    else:
        halos = [shift(halos[1], "row", 1), shift(halos[0], "row", -1)]

    slabs, first = call(
        functools.partial(slab_kernel, nr),
        (table, pixels, outside(weight), *halos),
        [pltpu.HBM((nc, places, width), video.dtype), bf16(patch // channels, half)],
        12,
        scratch=[
            VMEM((table.shape[2], width), video.dtype),
            VMEM((nc, places, width), video.dtype),
            pltpu.SemaphoreType.DMA((nc + 1,)),
        ],
        hbm=(2,),
        out_hbm=(0,),
        flops=2 * table.size * width,
    )
    slabs = lax.all_to_all(slabs, "col", 0, 0, tiled=True)

    ring = [(i + d, i + 1 - d) for i in range(1, nc - 1, 2) for d in range(2)]
    edge = lax.ppermute(edge, "col", ring)
    held, offsets = [tokens[None]], [2 * k for k in range(nc // 2)]
    for bit in offsets[1:]:
        held.append(swap(tokens[None], "col", bit))
    beside = swap(joined(held[:2]), "col", 1)
    others = [beside, swap(joined(held[2:]), "col", 1)]
    pieces = held + others

    keep, send, *rims = video_partials(first, weight, tokens, beside, edge, dims, channels)
    if nr == 2:
        rims = [swap(rims[0], "row", 1)]
    else:
        rims = [shift(rims[1], "row", 1), shift(rims[0], "row", -1)]
    keep, send = call(
        functools.partial(rim_kernel, (nm, nr)), (keep, send, *rims), [f32(*keep.shape), f32(*send.shape)], 6
    )
    video_grad = keep
    for s in range(1, nm):
        part = rotate(send[s - 1], "mp", s)
        video_grad = video_grad + part

    share = touched * KS
    (matrix,) = call(functools.partial(table_kernel, cols), (), [bf16(width + 128, KS * cols)], 4)
    (unfolded,) = call(
        functools.partial(unfold_kernel, (groups, cols, touched), tuple(offsets)),
        (slabs, spread, matrix),
        [bf16(nr, share, groups * nc * cols)],
        10,
        flops=2 * nc * groups * units * (width + 128) * KS * cols,
    )
    sums = [None] * nr
    for s in (*range(1, nr), 0):
        (mine,) = call(
            functools.partial(weight_kernel, (groups, cols, touched), s),
            (unfolded, *pieces),
            [f32(share, half)],
            8,
            scratch=[VMEM((half // 128, share, 128), jnp.float32)],
            flops=2 * share * groups * nc * cols * half,
        )
        if block % KS:
            mine = lax.dynamic_slice_in_dim(mine, ((r + s) % nr * nc + c) * block % KS, block, 0)
        sums[s] = rotate(mine, "row", s) if s else mine
    total = functools.reduce(jnp.add, sums)
    weight_grad = total * lax.rsqrt(jnp.float32(count * nr * nc))
    return video_grad, weight_grad


def solution(mesh):
    return jax.shard_map(
        both_gradients,
        mesh=mesh,
        in_specs=(P(None, None, "row", "col"), P(None, "row", "col", "mp"), P(None, "mp")),
        out_specs=(P(None, "mp", "row", "col"), P(("row", "col"), "mp")),
        check_vma=False,
    )
```
